512 devices in a mesh: node: 128 (over z, y, core), rep: 4 (over x).
Axes of the slice: x: 4, y: 8, z: 8, core: 2. Of those that a mesh axis runs over, the one named last changes fastest.
Arguments:
- coords: float32 [3, 65536], P(None, 'node'), may hold values from 0 to 2, as said below
- omega: bfloat16 [65536, 512], P('node', 'rep'), may hold values from -6 to 6
- skeleton: int32 [128, 256], P('node', 'rep'), may hold values from 0 to 65535, as said below
Outputs:
- row_sample: bfloat16 [65536, 512], P('node', 'rep')
- col_sample: float32 [65536, 512], P('node', 'rep')
The draws below stay inside these ranges and needn't reach their ends.
Inputs may be any that keep to these rules, and one draw needn't show every extreme that they name: `skeleton`: each node's list holds distinct indices, none inside its own points, at most 8 inside the points of any one other node; in every draw one node's points hold exactly 8 indices of every other node's list. `coords`: the first coordinate of point p lies between 2 (p // 512) / 128 and 2 (p // 512 + 1) / 128; the other two lie in [0, 1].
All inputs are finite; a program needn't handle non-finite values.
Results may differ from the reference program's by a relative error of at most 0.0049.
Values may be sent and summed in bfloat16 or wider, within the bound.
A program may use at most 128 MiB of HBM per device.

```python
import jax
import jax.numpy as jnp
from jax import lax

LEAF = 512
RANK = 256
SAMP = 512
NPTS = 65536
N_NODE = 128


def draw_coords(key, part):
    unit = jax.random.uniform(key, (3, N_NODE * LEAF), jnp.float32)
    leaf_ids = (jnp.arange(N_NODE * LEAF) // LEAF).astype(jnp.float32)
    first = 2.0 * (leaf_ids + unit[0]) / N_NODE
    others = unit[1:]
    return jnp.concatenate([first[None, :], others], axis=0).astype(jnp.float32)


def draw_skeleton(key, part):
    key_one, random_key_second, key_three, key_four, key_five = jax.random.split(key, 5)
    capacity = max(8, 2 * RANK // (N_NODE - 1))
    position_count = N_NODE * capacity
    node_ids = jnp.arange(N_NODE, dtype=jnp.int32)
    popular = jax.random.randint(key_one, (), 0, N_NODE, dtype=jnp.int32)
    filled_owner = jnp.where(node_ids == popular, (popular + 1) % N_NODE, popular)
    linear_index = jnp.arange(position_count, dtype=jnp.int32).reshape(1, N_NODE, capacity)
    holder_preference = jax.random.randint(random_key_second, (N_NODE,), 0, 3, dtype=jnp.int32) * 512
    unadjusted_score = jax.random.randint(key_three, (N_NODE, N_NODE, capacity), 0, 1024, dtype=jnp.int32)
    owner_ids = node_ids[None, :, None]
    ranking_score = (unadjusted_score + holder_preference[None, :, None]) * position_count + linear_index
    ranking_score = jnp.where(owner_ids == filled_owner[:, None, None], 3000 * position_count + linear_index, ranking_score)
    ranking_score = jnp.where(owner_ids == node_ids[:, None, None], -1 - linear_index, ranking_score)
    unused, chosen = lax.top_k(ranking_score.reshape(N_NODE, position_count), RANK)
    chosen_owner = chosen // capacity
    chosen_slot = chosen % capacity
    offset_base = jax.random.randint(key_four, (N_NODE, N_NODE), 0, LEAF, dtype=jnp.int32)
    stride_step = 2 * jax.random.randint(key_five, (N_NODE, N_NODE), 0, LEAF // 2, dtype=jnp.int32) + 1
    base_taken = jnp.take_along_axis(offset_base, chosen_owner, axis=1)
    stride_taken = jnp.take_along_axis(stride_step, chosen_owner, axis=1)
    local_index = (base_taken + chosen_slot * stride_taken) % LEAF
    return (chosen_owner * LEAF + local_index).astype(jnp.int32)


def block_levels(rng, shape, shards, smallest, high):
    gain, own = 1.0, jax.random.fold_in(rng, 6)
    for dim, blocks in shards:
        heights = jnp.exp(jax.random.uniform(jax.random.fold_in(own, dim), (blocks,), jnp.float32, smallest / len(shards), high / len(shards)))
        gain = gain * jnp.repeat(heights, shape[dim] // blocks).reshape([-1 if axis == dim else 1 for axis in range(len(shape))])
    return gain


def centred(own_key, dims, deviation, most, cuts=(), held_as=jnp.bfloat16):
    entries = deviation * jax.random.normal(own_key, dims, jnp.float32)
    if cuts:
        entries = entries * block_levels(own_key, dims, cuts, -0.22, 0.18)
    return jnp.clip(entries, -most, most).astype(held_as)


def setup_inputs(seed: int = 0) -> dict:
    splits = jax.random.split(jax.random.key(seed), 4)
    return {
        "coords": draw_coords(jax.random.fold_in(splits[3], 71), 0),
        "omega": centred(splits[1], (NPTS, SAMP), 1.0, 6.0, ((0, 128), (1, 4))),
        "skeleton": draw_skeleton(jax.random.fold_in(splits[3], 71), 0),
    }


kernel_scale = 0.0078125
softening = 0.02

def kernel_tile(first_points, target_points):
    squared = (first_points[0][:, None] - target_points[0][None, :]) ** 2
    squared = squared + (first_points[1][:, None] - target_points[1][None, :]) ** 2
    squared = squared + (first_points[2][:, None] - target_points[2][None, :]) ** 2
    return (kernel_scale * lax.rsqrt(squared + softening * softening)).astype(jnp.bfloat16)

def reference(coords, omega, skeleton):
    padded_points = jnp.pad(coords, ((0, 0), (LEAF, LEAF)))
    padded_rows = jnp.pad(omega, ((LEAF, LEAF), (0, 0)))

    def advance(col_total, node_index):
        start = (node_index * LEAF).astype(jnp.int32)
        own_points = lax.dynamic_slice_in_dim(coords, start, LEAF, 1)
        own_rows = lax.dynamic_slice_in_dim(omega, start, LEAF, 0)
        wide_points = lax.dynamic_slice_in_dim(padded_points, start, 3 * LEAF, 1)
        wide_rows = lax.dynamic_slice_in_dim(padded_rows, start, 3 * LEAF, 0)
        row_total = jnp.dot(kernel_tile(own_points, wide_points), wide_rows, preferred_element_type=jnp.float32)
        listed = skeleton[node_index]
        skel_tile = kernel_tile(own_points, coords[:, listed])
        row_total = row_total + jnp.dot(skel_tile, omega[listed], preferred_element_type=jnp.float32)
        transposed = lax.dot_general(skel_tile, own_rows, (((0,), (0,)), ((), ())), preferred_element_type=jnp.float32)
        col_total = col_total.at[listed].add(transposed)
        return (col_total, row_total.astype(jnp.bfloat16))
    col_total, blocked_rows = lax.scan(advance, jnp.zeros((N_NODE * LEAF, SAMP), jnp.float32), jnp.arange(N_NODE, dtype=jnp.int32))
    return (blocked_rows.reshape(N_NODE * LEAF, SAMP), col_total)
```

```python
import functools

import jax
import jax.numpy as jnp
from jax import lax
from jax.experimental import pallas as pl
from jax.experimental.pallas import tpu as pltpu
from jax.sharding import PartitionSpec as P

MESH = pl.DeviceIdType.MESH
kernel_scale = 0.0078125
softening = 0.02
CAP = 8
F32 = jnp.float32
BF16 = jnp.bfloat16


def dot(a, b):
    return jnp.dot(a, b, preferred_element_type=F32)


def dot_tn(a, b):
    return lax.dot_general(a, b, (((0,), (0,)), ((), ())), preferred_element_type=F32)


def dot_nt(a, b):
    return lax.dot_general(a, b, (((1,), (1,)), ((), ())), preferred_element_type=F32)


def iota(shape, dim):
    return lax.broadcasted_iota(jnp.int32, shape, dim)


def kernel_tile(columns, rows):
    squared = (columns[0] - rows[0]) ** 2
    squared = squared + (columns[1] - rows[1]) ** 2
    squared = squared + (columns[2] - rows[2]) ** 2
    return (kernel_scale * lax.rsqrt(squared + softening * softening)).astype(BF16)


def split3(values):
    high = values.astype(BF16).astype(F32)
    rest = values - high
    middle = rest.astype(BF16).astype(F32)
    return high, middle, rest - middle


def far_first(rows, cols):
    def wrapped(value, size):
        return (value + size // 2 - 1) % size - (size // 2 - 1)

    seen, groups = {(0, 0)}, []
    for a in range(rows):
        for b in range(cols):
            group = []
            for p, q in ((a, b), (-b, a), (-a, -b), (b, -a)):
                pair = (wrapped(p, rows), wrapped(q, cols))
                if pair not in seen:
                    seen.add(pair)
                    group.append(pair)
            if group:
                groups.append(group)
    groups.sort(key=lambda g: -(abs(g[0][0]) + abs(g[0][1])))
    return [pair for group in groups for pair in group]


def level_kernel(
    nodes, reps, coords_ref, omega_ref, skel_ref, row_ref, col_ref,
    lists, reqs, asked, cout, cin, rout, rin, pout, pin, nbc, nbw, own_t, acc, hot,
    send_sem, recv_sem, nb_send, nb_recv,
):
    me, rep = lax.axis_index("node"), lax.axis_index("rep")
    leaf = coords_ref.shape[1]
    samp = omega_ref.shape[1]
    share = skel_ref.shape[1]
    rank_size = share * reps
    slots = nodes * CAP
    z, y, core = me // 16, lax.rem(me // 2, 8), lax.rem(me, 2)
    offsets = far_first(8, 8)

    barrier = pltpu.get_barrier_semaphore()

    @pl.loop(1, reps)
    def _(d):
        pl.semaphore_signal(barrier, inc=1, device_id=(me, lax.rem(rep + d, reps)), device_id_type=MESH)

    @pl.loop(1, nodes)
    def _(d):
        pl.semaphore_signal(barrier, inc=1, device_id=(lax.rem(me + d, nodes), rep), device_id_type=MESH)

    own = coords_ref[...]
    own_rows = [own[k : k + 1, :] for k in range(3)]
    own_t[...] = jnp.transpose(
        jnp.concatenate([own, jnp.zeros((128 - 3, leaf), F32)], axis=0)
    )

    def near(point_rows, sample_rows, first):
        @pl.loop(0, leaf // 128)
        def _(m):
            part = pl.ds(pl.multiple_of(m * 128, 128), 128)
            columns = [own_t[part, k : k + 1] for k in range(3)]
            term = dot(kernel_tile(columns, point_rows), sample_rows)
            acc[part, :] = term if first else acc[part, :] + term

    near(own_rows, omega_ref[...], True)
    asked[me] = jnp.zeros((1, 128), F32)
    cin[me] = jnp.zeros((1, 128), F32)
    rin[me] = jnp.zeros((CAP, samp), BF16)
    pin[me] = jnp.zeros((CAP, samp), BF16)
    lists[rep] = skel_ref[...]

    pl.semaphore_wait(barrier, nodes - 1 + reps - 1)

    for d in range(1, reps):
        pltpu.make_async_remote_copy(
            src_ref=skel_ref, dst_ref=lists.at[rep], send_sem=send_sem.at[0], recv_sem=recv_sem.at[0],
            device_id=(me, lax.rem(rep + d, reps)), device_id_type=MESH,
        ).start()

    nb_copies = []
    for side, step in ((0, 1), (1, nodes - 1)):
        for j, (src, dst) in enumerate(((coords_ref, nbc), (omega_ref, nbw))):
            nb_copies.append(
                pltpu.make_async_remote_copy(
                    src_ref=src, dst_ref=dst.at[side], send_sem=nb_send.at[side, j], recv_sem=nb_recv.at[side, j],
                    device_id=(lax.rem(me + step, nodes), rep), device_id_type=MESH,
                )
            )
    for copy in nb_copies:
        copy.start()

    def await_bytes(ref, count, sem):
        view = ref.at[pl.ds(0, count)]
        pltpu.make_async_copy(view, view, sem).wait()

    def exchange(src, dst, which):
        def send(target):
            pltpu.make_async_remote_copy(
                src_ref=src.at[target], dst_ref=dst.at[me], send_sem=send_sem.at[which], recv_sem=recv_sem.at[which],
                device_id=(target, rep), device_id_type=MESH,
            ).start()

        for dy, dz in offsets:
            base = lax.rem(z + (dz + 8), 8) * 16 + lax.rem(y + (dy + 8), 8) * 2
            send(base + core)
            send(base + 1 - core)
        send(z * 16 + y * 2 + 1 - core)

    await_bytes(lists, reps - 1, recv_sem.at[0])

    listed = jnp.concatenate([lists[r] for r in range(reps)], axis=1)
    owner_row = listed >> 9
    listed_col = jnp.transpose(jnp.broadcast_to(listed.astype(F32), (128, rank_size))).astype(jnp.int32)
    owner_col = listed_col >> 9
    value_col = (listed_col & (leaf - 1)) + 1
    wide_owner = jnp.concatenate([owner_col] * (rank_size // 128), axis=1)
    same = wide_owner == owner_row
    before = jnp.where(same & (iota(same.shape, 1) < iota(same.shape, 0)), 1.0, 0.0).astype(BF16)
    rank_col = dot(before, jnp.ones((rank_size, 128), BF16)).astype(jnp.int32)
    placed = rank_col == iota((rank_size, 128), 1)
    owner_hot = jnp.where(owner_row == iota((nodes, rank_size), 0), 1.0, 0.0).astype(BF16)
    low = jnp.where(placed, (value_col & 255).astype(F32), 0.0).astype(BF16)
    high = jnp.where(placed, (value_col >> 8).astype(F32), 0.0).astype(BF16)
    request = dot(owner_hot, low) + 256.0 * dot(owner_hot, high)
    reqs[...] = request.reshape(nodes, 1, 128)
    exchange(reqs, asked, 1)

    for copy in nb_copies:
        copy.wait_recv()

    @pl.when(me > 0)
    def _():
        side = nbc[0]
        near([side[k : k + 1, :] for k in range(3)], nbw[0], False)

    @pl.when(me < nodes - 1)
    def _():
        side = nbc[1]
        near([side[k : k + 1, :] for k in range(3)], nbw[1], False)

    parts = []
    for k in range(3):
        parts += list(split3(own_rows[k]))
    stack = jnp.concatenate([jnp.concatenate(parts[3 * k : 3 * k + 3] * CAP, axis=0) for k in range(3)], axis=0)
    stack = jnp.concatenate([stack, jnp.zeros((128 - 9 * CAP, leaf), F32)], axis=0)
    lane = iota((128, leaf), 0)
    slot_of = lax.rem(lane, 24) // 3
    tables = [jnp.where(slot_of == s, stack, 0.0).astype(BF16) for s in range(CAP)]

    await_bytes(asked, nodes - 1, recv_sem.at[1])

    wanted = asked[...].reshape(nodes, 128)
    point = (iota((nodes, leaf), 1) + 1).astype(F32)
    answer = jnp.zeros((nodes, 128), F32)
    for s in range(CAP):
        slot_hot = jnp.where(wanted[:, s : s + 1] == point, 1.0, 0.0).astype(BF16)
        answer = answer + dot_nt(slot_hot, tables[s])
    cout[...] = answer.reshape(nodes, 1, 128)
    exchange(cout, cin, 2)

    spread = jnp.broadcast_to(asked[...], (nodes, CAP, 128))
    spread = jnp.where(iota(spread.shape, 2) == iota(spread.shape, 1), spread, 0.0)
    flat = jnp.sum(spread.reshape(slots, 128), axis=1, keepdims=True)
    hot[...] = jnp.where(flat == (iota((slots, leaf), 1) + 1).astype(F32), 1.0, 0.0).astype(BF16)
    rows = dot(hot[...], omega_ref[...])
    rout[...] = rows.reshape(nodes, CAP, samp).astype(BF16)
    exchange(rout, rin, 3)

    flat_col = owner_col * CAP + rank_col
    flat_wide = jnp.concatenate([flat_col] * (slots // 128), axis=1)
    gather_hot = jnp.where(flat_wide == iota((rank_size, slots), 1), 1.0, 0.0).astype(BF16)
    earlier = jnp.where(same & (iota(same.shape, 0) < iota(same.shape, 1)), 1.0, 0.0)
    rank_row = jnp.sum(earlier, axis=0, keepdims=True).astype(jnp.int32)
    flat_row = owner_row * CAP + rank_row
    scatter_hot = jnp.where(flat_row == iota((slots, rank_size), 0), 1.0, 0.0).astype(BF16)
    pick = jnp.where(owner_col == iota((rank_size, 128), 1), 1.0, 0.0).astype(BF16)
    lanes = iota((rank_size, 128), 1)
    mine = lax.rem(lanes, 24) // 3 == rank_col

    await_bytes(cin, nodes - 1, recv_sem.at[2])
    found = dot(pick, cin[...].reshape(nodes, 128).astype(BF16))
    skel_cols = [
        jnp.sum(jnp.where(mine & (lanes // 24 == k), found, 0.0), axis=1, keepdims=True) for k in range(3)
    ]
    skel_tile = kernel_tile(skel_cols, own_rows)
    transposed = dot(skel_tile, omega_ref[...]).astype(BF16)
    pout[...] = dot(scatter_hot, transposed).reshape(nodes, CAP, samp).astype(BF16)
    exchange(pout, pin, 4)

    await_bytes(rin, nodes - 1, recv_sem.at[3])
    got = rin[...].astype(F32).reshape(slots, samp).astype(BF16)
    skel_samples = dot(gather_hot, got).astype(BF16)
    row_ref[...] = (acc[...] + dot_tn(skel_tile, skel_samples)).astype(BF16)

    await_bytes(pin, nodes - 1, recv_sem.at[4])
    incoming = pin[...].astype(F32).reshape(slots, samp).astype(BF16)
    col_ref[...] = dot_tn(hot[...], incoming)

    await_bytes(lists, reps - 1, send_sem.at[0])
    for which, ref in ((1, reqs), (2, cout), (3, rout), (4, pout)):
        await_bytes(ref, nodes - 1, send_sem.at[which])
    for copy in nb_copies:
        copy.wait_send()


def solution(mesh):
    nodes, reps = mesh.shape["node"], mesh.shape["rep"]

    def on_device(coords, omega, skeleton):
        leaf, samp = omega.shape
        share = skeleton.shape[1]
        vmem = pl.BlockSpec(memory_space=pltpu.VMEM)
        return pl.pallas_call(
            functools.partial(level_kernel, nodes, reps),
            out_shape=(
                jax.ShapeDtypeStruct((leaf, samp), BF16),
                jax.ShapeDtypeStruct((leaf, samp), F32),
            ),
            in_specs=[vmem] * 3,
            out_specs=(vmem, vmem),
            scratch_shapes=[
                pltpu.VMEM((reps, 1, share), jnp.int32),
                pltpu.VMEM((nodes, 1, 128), F32),
                pltpu.VMEM((nodes, 1, 128), F32),
                pltpu.VMEM((nodes, 1, 128), F32),
                pltpu.VMEM((nodes, 1, 128), F32),
                pltpu.VMEM((nodes, CAP, samp), BF16),
                pltpu.VMEM((nodes, CAP, samp), BF16),
                pltpu.VMEM((nodes, CAP, samp), BF16),
                pltpu.VMEM((nodes, CAP, samp), BF16),
                pltpu.VMEM((2, 3, leaf), F32),
                pltpu.VMEM((2, leaf, samp), BF16),
                pltpu.VMEM((leaf, 128), F32),
                pltpu.VMEM((leaf, samp), F32),
                pltpu.VMEM((nodes * CAP, leaf), BF16),
                pltpu.SemaphoreType.DMA((5,)),
                pltpu.SemaphoreType.DMA((5,)),
                pltpu.SemaphoreType.DMA((2, 2)),
                pltpu.SemaphoreType.DMA((2, 2)),
            ],
            compiler_params=pltpu.CompilerParams(collective_id=0, has_side_effects=True),
        )(coords, omega, skeleton)

    return jax.shard_map(
        on_device,
        mesh=mesh,
        in_specs=(P(None, "node"), P("node", "rep"), P("node", "rep")),
        out_specs=(P("node", "rep"), P("node", "rep")),
        check_vma=False,
    )
```

```python
import functools

import jax
import jax.numpy as jnp
from jax import lax
from jax.experimental import pallas as pl
from jax.experimental.pallas import tpu as pltpu
from jax.sharding import PartitionSpec as P

MESH = pl.DeviceIdType.MESH
kernel_scale = 0.0078125
softening = 0.02
CAP = 8
VMEM_LIMIT = 24 << 20
F32 = jnp.float32
BF16 = jnp.bfloat16


def dot(a, b):
    return jnp.dot(a, b, preferred_element_type=F32)


def dot_tn(a, b):
    return lax.dot_general(a, b, (((0,), (0,)), ((), ())), preferred_element_type=F32)


def dot_nt(a, b):
    return lax.dot_general(a, b, (((1,), (1,)), ((), ())), preferred_element_type=F32)


def iota(shape, dim):
    return lax.broadcasted_iota(jnp.int32, shape, dim)


def kernel_tile(columns, rows):
    squared = (columns[0] - rows[0]) ** 2
    squared = squared + (columns[1] - rows[1]) ** 2
    squared = squared + (columns[2] - rows[2]) ** 2
    return (kernel_scale * lax.rsqrt(squared + softening * softening)).astype(BF16)


def split3(values):
    high = values.astype(BF16).astype(F32)
    rest = values - high
    middle = rest.astype(BF16).astype(F32)
    return high, middle, rest - middle


def far_first(rows, cols):
    def wrapped(value, size):
        return (value + size // 2 - 1) % size - (size // 2 - 1)

    seen, groups = {(0, 0)}, []
    for a in range(rows):
        for b in range(cols):
            group = []
            for p, q in ((a, b), (-b, a), (-a, -b), (b, -a)):
                pair = (wrapped(p, rows), wrapped(q, cols))
                if pair not in seen:
                    seen.add(pair)
                    group.append(pair)
            if group:
                groups.append(group)
    groups.sort(key=lambda g: -(abs(g[0][0]) + abs(g[0][1])))
    return [pair for group in groups for pair in group]


def level_kernel(
    nodes, reps, coords_hbm, omega_hbm, skel_hbm, row_ref, pin, spots,
    coords_ref, omega_ref, skel_ref, lists, reqs, asked, cout, cin, rout, rin, pout, nbc, nbw, own_t, acc, hot,
    load_sem, plane_sem, send_sem, recv_sem, nb_send, nb_recv,
):
    me, rep = lax.axis_index("node"), lax.axis_index("rep")
    leaf = coords_ref.shape[1]
    samp = omega_ref.shape[1]
    share = skel_ref.shape[1]
    rank_size = share * reps
    slots = nodes * CAP
    z, y, core = me // 16, lax.rem(me // 2, 8), lax.rem(me, 2)
    offsets = far_first(8, 8)

    barrier = pltpu.get_barrier_semaphore()

    @pl.loop(1, reps)
    def _(d):
        pl.semaphore_signal(barrier, inc=1, device_id=(me, lax.rem(rep + d, reps)), device_id_type=MESH)

    @pl.loop(1, 8)
    def _(d):
        pl.semaphore_signal(barrier, inc=1, device_id=(lax.rem(me + 16 * d, nodes), rep), device_id_type=MESH)

    @pl.loop(1, 16)
    def _(d):
        peer = z * 16 + lax.rem(lax.rem(me, 16) + d, 16)
        pl.semaphore_signal(barrier, inc=1, device_id=(peer, rep), device_id_type=MESH)

    loads = [
        pltpu.make_async_copy(src, dst, load_sem.at[k])
        for k, (src, dst) in enumerate(((skel_hbm, skel_ref), (coords_hbm, coords_ref), (omega_hbm, omega_ref)))
    ]
    for load in loads:
        load.start()
    for load in loads:
        load.wait()

    own = coords_ref[...]
    own_rows = [own[k : k + 1, :] for k in range(3)]
    own_t[...] = jnp.transpose(
        jnp.concatenate([own, jnp.zeros((128 - 3, leaf), F32)], axis=0)
    )

    def near(point_rows, sample_rows, first):
        @pl.loop(0, leaf // 128)
        def _(m):
            part = pl.ds(pl.multiple_of(m * 128, 128), 128)
            columns = [own_t[part, k : k + 1] for k in range(3)]
            term = dot(kernel_tile(columns, point_rows), sample_rows)
            acc[part, :] = term if first else acc[part, :] + term

    near(own_rows, omega_ref[...], True)
    asked[me] = jnp.zeros((1, 128), F32)
    cin[me] = jnp.zeros((1, 128), F32)
    rin[me] = jnp.zeros((CAP, samp), BF16)
    pin[me] = jnp.zeros((CAP, samp), BF16)
    lists[rep] = skel_ref[...]

    pl.semaphore_wait(barrier, reps - 1 + 7 + 15)

    for d in range(1, reps):
        pltpu.make_async_remote_copy(
            src_ref=skel_ref, dst_ref=lists.at[rep], send_sem=send_sem.at[0], recv_sem=recv_sem.at[0],
            device_id=(me, lax.rem(rep + d, reps)), device_id_type=MESH,
        ).start()

    nb_copies = []
    for side, step in ((0, 1), (1, nodes - 1)):
        for j, (src, dst) in enumerate(((coords_ref, nbc), (omega_ref, nbw))):
            nb_copies.append(
                pltpu.make_async_remote_copy(
                    src_ref=src, dst_ref=dst.at[side], send_sem=nb_send.at[side, j], recv_sem=nb_recv.at[side, j],
                    device_id=(lax.rem(me + step, nodes), rep), device_id_type=MESH,
                )
            )

    @pl.loop(1, 8)
    def _(d):
        pl.semaphore_signal(plane_sem, inc=1, device_id=(lax.rem(me + 16 * d, nodes), rep), device_id_type=MESH)

    def await_bytes(ref, count, sem):
        view = ref.at[pl.ds(0, count)]
        pltpu.make_async_copy(view, view, sem).wait()

    def exchange(src, dst, which):
        def send(target):
            pltpu.make_async_remote_copy(
                src_ref=src.at[target], dst_ref=dst.at[me], send_sem=send_sem.at[which], recv_sem=recv_sem.at[which],
                device_id=(target, rep), device_id_type=MESH,
            ).start()

        for dy, dz in offsets:
            base = lax.rem(z + (dz + 8), 8) * 16 + lax.rem(y + (dy + 8), 8) * 2
            send(base + core)
            send(base + 1 - core)
        send(z * 16 + y * 2 + 1 - core)

    await_bytes(lists, reps - 1, recv_sem.at[0])

    listed = jnp.concatenate([lists[r] for r in range(reps)], axis=1)
    owner_row = listed >> 9
    listed_col = jnp.transpose(jnp.broadcast_to(listed.astype(F32), (128, rank_size))).astype(jnp.int32)
    owner_col = listed_col >> 9
    value_col = (listed_col & (leaf - 1)) + 1
    wide_owner = jnp.concatenate([owner_col] * (rank_size // 128), axis=1)
    same = wide_owner == owner_row
    before = jnp.where(same & (iota(same.shape, 1) < iota(same.shape, 0)), 1.0, 0.0).astype(BF16)
    rank_col = dot(before, jnp.ones((rank_size, 128), BF16)).astype(jnp.int32)
    placed = rank_col == iota((rank_size, 128), 1)
    owner_hot = jnp.where(owner_row == iota((nodes, rank_size), 0), 1.0, 0.0).astype(BF16)
    low = jnp.where(placed, (value_col & 255).astype(F32), 0.0).astype(BF16)
    high = jnp.where(placed, (value_col >> 8).astype(F32), 0.0).astype(BF16)
    request = dot(owner_hot, low) + 256.0 * dot(owner_hot, high)
    reqs[...] = request.reshape(nodes, 1, 128)
    pl.semaphore_wait(plane_sem, 7)
    exchange(reqs, asked, 1)
    for copy in nb_copies:
        copy.start()

    parts = []
    for k in range(3):
        parts += list(split3(own_rows[k]))
    stack = jnp.concatenate([jnp.concatenate(parts[3 * k : 3 * k + 3] * CAP, axis=0) for k in range(3)], axis=0)
    stack = jnp.concatenate([stack, jnp.zeros((128 - 9 * CAP, leaf), F32)], axis=0)
    lane = iota((128, leaf), 0)
    slot_of = lax.rem(lane, 24) // 3
    tables = [jnp.where(slot_of == s, stack, 0.0).astype(BF16) for s in range(CAP)]

    for copy in nb_copies:
        copy.wait_recv()

    @pl.when(me > 0)
    def _():
        side = nbc[0]
        near([side[k : k + 1, :] for k in range(3)], nbw[0], False)

    await_bytes(asked, nodes - 1, recv_sem.at[1])

    wanted = asked[...].reshape(nodes, 128)
    point = (iota((nodes, leaf), 1) + 1).astype(F32)
    answer = jnp.zeros((nodes, 128), F32)
    for s in range(CAP):
        slot_hot = jnp.where(wanted[:, s : s + 1] == point, 1.0, 0.0).astype(BF16)
        answer = answer + dot_nt(slot_hot, tables[s])
    cout[...] = answer.reshape(nodes, 1, 128)
    exchange(cout, cin, 2)

    spread = jnp.broadcast_to(asked[...], (nodes, CAP, 128))
    spread = jnp.where(iota(spread.shape, 2) == iota(spread.shape, 1), spread, 0.0)
    flat = jnp.sum(spread.reshape(slots, 128), axis=1, keepdims=True)
    hot[...] = jnp.where(flat == (iota((slots, leaf), 1) + 1).astype(F32), 1.0, 0.0).astype(BF16)
    rows = dot(hot[...], omega_ref[...])
    rout[...] = rows.reshape(nodes, CAP, samp).astype(BF16)
    exchange(rout, rin, 3)

    flat_col = owner_col * CAP + rank_col
    flat_wide = jnp.concatenate([flat_col] * (slots // 128), axis=1)
    gather_hot = jnp.where(flat_wide == iota((rank_size, slots), 1), 1.0, 0.0).astype(BF16)
    earlier = jnp.where(same & (iota(same.shape, 0) < iota(same.shape, 1)), 1.0, 0.0)
    rank_row = jnp.sum(earlier, axis=0, keepdims=True).astype(jnp.int32)
    flat_row = owner_row * CAP + rank_row
    scatter_hot = jnp.where(flat_row == iota((slots, rank_size), 0), 1.0, 0.0).astype(BF16)
    pick = jnp.where(owner_col == iota((rank_size, 128), 1), 1.0, 0.0).astype(BF16)
    lanes = iota((rank_size, 128), 1)
    mine = lax.rem(lanes, 24) // 3 == rank_col

    @pl.when(me < nodes - 1)
    def _():
        side = nbc[1]
        near([side[k : k + 1, :] for k in range(3)], nbw[1], False)

    await_bytes(cin, nodes - 1, recv_sem.at[2])
    found = dot(pick, cin[...].reshape(nodes, 128).astype(BF16))
    skel_cols = [
        jnp.sum(jnp.where(mine & (lanes // 24 == k), found, 0.0), axis=1, keepdims=True) for k in range(3)
    ]
    skel_tile = kernel_tile(skel_cols, own_rows)
    transposed = dot(skel_tile, omega_ref[...]).astype(BF16)
    pout[...] = dot(scatter_hot, transposed).reshape(nodes, CAP, samp).astype(BF16)
    exchange(pout, pin, 4)
    spots[...] = jnp.transpose(hot[...])

    await_bytes(rin, nodes - 1, recv_sem.at[3])
    got = rin[...].astype(F32).reshape(slots, samp).astype(BF16)
    skel_samples = dot(gather_hot, got).astype(BF16)
    row_ref[...] = (acc[...] + dot_tn(skel_tile, skel_samples)).astype(BF16)

    await_bytes(lists, reps - 1, send_sem.at[0])
    for which, ref in ((1, reqs), (2, cout), (3, rout), (4, pout)):
        await_bytes(ref, nodes - 1, send_sem.at[which])
    for copy in nb_copies:
        copy.wait_send()
    await_bytes(pin, nodes - 1, recv_sem.at[4])


def finish_kernel(row_ref, pin, spots, row_hbm, col_hbm, incoming, col_ref, sems):
    leaf = row_ref.shape[0]
    copies = [pltpu.make_async_copy(row_ref, row_hbm, sems.at[0])]
    copies[0].start()
    incoming[...] = pin[...].astype(F32).reshape(incoming.shape).astype(BF16)
    step = leaf // 2
    for k in range(2):
        part = pl.ds(k * step, step)
        col_ref[part, :] = dot(spots[part, :], incoming[...])
        copies.append(pltpu.make_async_copy(col_ref.at[part], col_hbm.at[part], sems.at[1 + k]))
        copies[-1].start()
    for copy in copies:
        copy.wait()


def solution(mesh):
    nodes, reps = mesh.shape["node"], mesh.shape["rep"]

    def on_device(coords, omega, skeleton):
        leaf, samp = omega.shape
        share = skeleton.shape[1]
        vmem = pl.BlockSpec(memory_space=pltpu.VMEM)
        anywhere = pl.BlockSpec(memory_space=pl.ANY)
        row, incoming, spots = pl.pallas_call(
            functools.partial(level_kernel, nodes, reps),
            out_shape=(
                jax.ShapeDtypeStruct((leaf, samp), BF16),
                jax.ShapeDtypeStruct((nodes, CAP, samp), BF16),
                jax.ShapeDtypeStruct((leaf, nodes * CAP), BF16),
            ),
            in_specs=[pl.BlockSpec(memory_space=pltpu.HBM)] * 3,
            out_specs=(vmem,) * 3,
            scratch_shapes=[
                pltpu.VMEM(coords.shape, F32),
                pltpu.VMEM((leaf, samp), BF16),
                pltpu.VMEM((1, share), jnp.int32),
                pltpu.VMEM((reps, 1, share), jnp.int32),
                pltpu.VMEM((nodes, 1, 128), F32),
                pltpu.VMEM((nodes, 1, 128), F32),
                pltpu.VMEM((nodes, 1, 128), F32),
                pltpu.VMEM((nodes, 1, 128), F32),
                pltpu.VMEM((nodes, CAP, samp), BF16),
                pltpu.VMEM((nodes, CAP, samp), BF16),
                pltpu.VMEM((nodes, CAP, samp), BF16),
                pltpu.VMEM((2, 3, leaf), F32),
                pltpu.VMEM((2, leaf, samp), BF16),
                pltpu.VMEM((leaf, 128), F32),
                pltpu.VMEM((leaf, samp), F32),
                pltpu.VMEM((nodes * CAP, leaf), BF16),
                pltpu.SemaphoreType.DMA((3,)),
                pltpu.SemaphoreType.REGULAR,
                pltpu.SemaphoreType.DMA((5,)),
                pltpu.SemaphoreType.DMA((5,)),
                pltpu.SemaphoreType.DMA((2, 2)),
                pltpu.SemaphoreType.DMA((2, 2)),
            ],
            compiler_params=pltpu.CompilerParams(
                collective_id=0, has_side_effects=True, vmem_limit_bytes=VMEM_LIMIT
            ),
        )(coords, omega, skeleton)
        return pl.pallas_call(
            finish_kernel,
            out_shape=(
                jax.ShapeDtypeStruct((leaf, samp), BF16),
                jax.ShapeDtypeStruct((leaf, samp), F32),
            ),
            in_specs=[vmem] * 3,
            out_specs=(anywhere,) * 2,
            scratch_shapes=[
                pltpu.VMEM((nodes * CAP, samp), BF16),
                pltpu.VMEM((leaf, samp), F32),
                pltpu.SemaphoreType.DMA((3,)),
            ],
            compiler_params=pltpu.CompilerParams(vmem_limit_bytes=VMEM_LIMIT),
        )(row, incoming, spots)

    return jax.shard_map(
        on_device,
        mesh=mesh,
        in_specs=(P(None, "node"), P("node", "rep"), P("node", "rep")),
        out_specs=(P("node", "rep"), P("node", "rep")),
        check_vma=False,
    )
```

```python
import functools

import jax
import jax.numpy as jnp
from jax import lax
from jax.experimental import pallas as pl
from jax.experimental.pallas import tpu as pltpu
from jax.sharding import PartitionSpec as P

MESH = pl.DeviceIdType.MESH
kernel_scale = 0.0078125
softening = 0.02
CAP = 8
LINE = 16
Y_ORDER = (8, 7, 9, 6, 10, 5, 11, 4, 12, 3, 13, 2, 14, 1, 15)
Z_ORDER = (4, 3, 5, 2, 6, 1, 7)
ROWS_FIRST = True
VMEM_LIMIT = 24 << 20
F32 = jnp.float32
BF16 = jnp.bfloat16


def dot(a, b):
    return jnp.dot(a, b, preferred_element_type=F32)


def dot_tn(a, b):
    return lax.dot_general(a, b, (((0,), (0,)), ((), ())), preferred_element_type=F32)


def dot_nt(a, b):
    return lax.dot_general(a, b, (((1,), (1,)), ((), ())), preferred_element_type=F32)


def iota(shape, dim):
    return lax.broadcasted_iota(jnp.int32, shape, dim)


def kernel_tile(columns, rows):
    squared = (columns[0] - rows[0]) ** 2
    squared = squared + (columns[1] - rows[1]) ** 2
    squared = squared + (columns[2] - rows[2]) ** 2
    return (kernel_scale * lax.rsqrt(squared + softening * softening)).astype(BF16)


def split3(values):
    high = values.astype(BF16).astype(F32)
    rest = values - high
    middle = rest.astype(BF16).astype(F32)
    return high, middle, rest - middle


def far_first(rows, cols):
    def wrapped(value, size):
        return (value + size // 2 - 1) % size - (size // 2 - 1)

    seen, groups = {(0, 0)}, []
    for a in range(rows):
        for b in range(cols):
            group = []
            for p, q in ((a, b), (-b, a), (-a, -b), (b, -a)):
                pair = (wrapped(p, rows), wrapped(q, cols))
                if pair not in seen:
                    seen.add(pair)
                    group.append(pair)
            if group:
                groups.append(group)
    groups.sort(key=lambda g: -(abs(g[0][0]) + abs(g[0][1])))
    return [pair for group in groups for pair in group]


def level_kernel(
    nodes, reps, coords_hbm, omega_hbm, skel_hbm, row_ref, pin, spots,
    coords_ref, omega_ref, skel_ref, lists, reqs, asked, zreq, zasked, zout, zin, line, rout, rin, pout,
    nbc, nbw, own_t, own_wide, omega_t, table, acc, hot, scatter_hot, tile,
    load_sem, plane_sem, send_sem, recv_sem, nb_send, nb_recv,
):
    me, rep = lax.axis_index("node"), lax.axis_index("rep")
    leaf = coords_ref.shape[1]
    samp = omega_ref.shape[1]
    share = skel_ref.shape[1]
    rank_size = share * reps
    slots = nodes * CAP
    z, y, core = me // LINE, lax.rem(me // 2, LINE // 2), lax.rem(me, 2)
    spot = lax.rem(me, LINE)
    planes = nodes // LINE
    offsets = far_first(8, 8)

    def z_peer(d):
        return lax.rem(z + d, planes)

    def y_peer(d):
        return z * LINE + lax.rem(spot + d, LINE)

    barrier = pltpu.get_barrier_semaphore()

    @pl.loop(1, reps)
    def _(d):
        pl.semaphore_signal(barrier, inc=1, device_id=(me, lax.rem(rep + d, reps)), device_id_type=MESH)

    @pl.loop(1, LINE)
    def _(d):
        pl.semaphore_signal(barrier, inc=1, device_id=(y_peer(d), rep), device_id_type=MESH)

    @pl.loop(1, planes)
    def _(d):
        pl.semaphore_signal(barrier, inc=1, device_id=(z_peer(d) * LINE + spot, rep), device_id_type=MESH)

    loads = [
        pltpu.make_async_copy(src, dst, load_sem.at[k])
        for k, (src, dst) in enumerate(((skel_hbm, skel_ref), (coords_hbm, coords_ref), (omega_hbm, omega_ref)))
    ]
    for load in loads:
        load.start()
    loads[0].wait()
    loads[1].wait()
    pl.semaphore_wait(barrier, reps - 1 + LINE - 1 + planes - 1)

    for d in range(1, reps):
        pltpu.make_async_remote_copy(
            src_ref=skel_ref, dst_ref=lists.at[rep], send_sem=send_sem.at[0], recv_sem=recv_sem.at[0],
            device_id=(me, lax.rem(rep + d, reps)), device_id_type=MESH,
        ).start()
    for d in Y_ORDER:
        pltpu.make_async_remote_copy(
            src_ref=coords_ref, dst_ref=line.at[spot], send_sem=send_sem.at[5], recv_sem=recv_sem.at[5],
            device_id=(y_peer(d), rep), device_id_type=MESH,
        ).start()

    @pl.loop(1, planes)
    def _(d):
        pl.semaphore_signal(plane_sem, inc=1, device_id=(z_peer(d) * LINE + spot, rep), device_id_type=MESH)

    loads[2].wait()
    lists[rep] = skel_ref[...]
    line[spot] = coords_ref[...]
    asked[me] = jnp.zeros((1, 128), F32)
    rin[me] = jnp.zeros((CAP, samp), BF16)
    pin[me] = jnp.zeros((CAP, samp), BF16)
    own = coords_ref[...]
    own_rows = [own[k : k + 1, :] for k in range(3)]
    own_t[...] = jnp.transpose(jnp.concatenate([own, jnp.zeros((128 - 3, leaf), F32)], axis=0))
    for k in range(3):
        own_wide[k] = jnp.broadcast_to(own_t[:, k : k + 1], (leaf, 128))

    def near(point_rows, sample_rows, first):
        @pl.loop(0, leaf // 128)
        def _(m):
            part = pl.ds(pl.multiple_of(m * 128, 128), 128)
            columns = [jnp.concatenate([own_wide[k, part, :]] * (leaf // 128), axis=1) for k in range(3)]
            term = dot(kernel_tile(columns, point_rows), sample_rows)
            acc[part, :] = term if first else acc[part, :] + term

    near(own_rows, omega_ref[...], True)

    nb_copies = []
    for side, step in ((0, 1), (1, nodes - 1)):
        for j, (src, dst) in enumerate(((coords_ref, nbc), (omega_ref, nbw))):
            nb_copies.append(
                pltpu.make_async_remote_copy(
                    src_ref=src, dst_ref=dst.at[side], send_sem=nb_send.at[side, j], recv_sem=nb_recv.at[side, j],
                    device_id=(lax.rem(me + step, nodes), rep), device_id_type=MESH,
                )
            )

    def await_bytes(ref, count, sem):
        view = ref.at[pl.ds(0, count)]
        pltpu.make_async_copy(view, view, sem).wait()

    def exchange(src, dst, which):
        def send(target):
            pltpu.make_async_remote_copy(
                src_ref=src.at[target], dst_ref=dst.at[me], send_sem=send_sem.at[which], recv_sem=recv_sem.at[which],
                device_id=(target, rep), device_id_type=MESH,
            ).start()

        for dy, dz in offsets:
            base = lax.rem(z + (dz + 8), 8) * LINE + lax.rem(y + (dy + 8), 8) * 2
            send(base + core)
            send(base + 1 - core)
        send(z * LINE + y * 2 + 1 - core)

    def z_exchange(src, dst, which):
        for d in Z_ORDER:
            pltpu.make_async_remote_copy(
                src_ref=src.at[z_peer(d)], dst_ref=dst.at[z], send_sem=send_sem.at[which], recv_sem=recv_sem.at[which],
                device_id=(z_peer(d) * LINE + spot, rep), device_id_type=MESH,
            ).start()

    await_bytes(lists, reps - 1, recv_sem.at[0])

    listed = jnp.concatenate([lists[r] for r in range(reps)], axis=1)
    owner_row = listed >> 9
    listed_col = jnp.transpose(jnp.broadcast_to(listed.astype(F32), (128, rank_size))).astype(jnp.int32)
    owner_col = listed_col >> 9
    value_col = (listed_col & (leaf - 1)) + 1
    wide_owner = jnp.concatenate([owner_col] * (rank_size // 128), axis=1)
    same = wide_owner == owner_row
    before = jnp.where(same & (iota(same.shape, 1) < iota(same.shape, 0)), 1.0, 0.0).astype(BF16)
    rank_col = dot(before, jnp.ones((rank_size, 128), BF16)).astype(jnp.int32)
    low_col = (value_col & 255).astype(F32)
    high_col = (value_col >> 8).astype(F32)

    def requests(lane_col, owner_hot):
        placed = lane_col == iota((rank_size, 128), 1)
        low = jnp.where(placed, low_col, 0.0).astype(BF16)
        high = jnp.where(placed, high_col, 0.0).astype(BF16)
        return dot(owner_hot, low) + 256.0 * dot(owner_hot, high)

    z_hot = jnp.where((owner_row >> 4) == iota((16, rank_size), 0), 1.0, 0.0).astype(BF16)
    z_request = requests((owner_col & (LINE - 1)) * CAP + rank_col, z_hot)
    for i in range(planes):
        zreq[i] = z_request[i : i + 1, :]
    z_exchange(zreq, zasked, 2)
    zasked[z] = zreq[z]

    owner_hot = jnp.where(owner_row == iota((nodes, rank_size), 0), 1.0, 0.0).astype(BF16)
    reqs[...] = requests(rank_col, owner_hot).reshape(nodes, 1, 128)
    pl.semaphore_wait(plane_sem, planes - 1)
    exchange(reqs, asked, 1)
    for copy in nb_copies:
        copy.start()

    await_bytes(line, LINE - 1, recv_sem.at[5])
    for k in range(3):
        for part, values in enumerate(split3(jnp.concatenate([line[n, k : k + 1, :] for n in range(LINE)], axis=0))):
            table[pl.ds((3 * k + part) * LINE, LINE), :] = values.astype(BF16)

    await_bytes(zasked, planes - 1, recv_sem.at[2])
    width = 256
    for c in range(slots // width):
        wanted = jnp.concatenate([zasked[2 * c], zasked[2 * c + 1]], axis=1)
        point_hot = jnp.where(wanted == (iota((leaf, width), 0) + 1).astype(F32), 1.0, 0.0).astype(BF16)
        found = dot(table[...], point_hot)
        own_node = lax.rem(iota((3 * LINE, width), 0), LINE) == lax.rem(iota((3 * LINE, width), 1) // CAP, LINE)
        answer = jnp.concatenate(
            [
                jnp.sum(jnp.where(own_node, found[3 * LINE * k : 3 * LINE * (k + 1)], 0.0), axis=0, keepdims=True)
                for k in range(3)
            ],
            axis=0,
        )
        zout[2 * c] = answer[:, :128]
        zout[2 * c + 1] = answer[:, 128:]
    z_exchange(zout, zin, 6)
    zin[z] = zout[z]

    flat_col = owner_col * CAP + rank_col
    flat_wide = jnp.concatenate([flat_col] * (slots // 128), axis=1)
    gather_hot = jnp.where(flat_wide == iota((rank_size, slots), 1), 1.0, 0.0).astype(BF16)
    earlier = jnp.where(same & (iota(same.shape, 0) < iota(same.shape, 1)), 1.0, 0.0)
    rank_row = jnp.sum(earlier, axis=0, keepdims=True).astype(jnp.int32)
    flat_row = owner_row * CAP + rank_row
    scatter_hot[...] = jnp.where(flat_row == iota((slots, rank_size), 0), 1.0, 0.0).astype(BF16)

    for copy in nb_copies:
        copy.wait_recv()
    omega_t[...] = jnp.transpose(omega_ref[...])

    @pl.when(me > 0)
    def _():
        side = nbc[0]
        near([side[k : k + 1, :] for k in range(3)], nbw[0], False)

    @pl.when(me < nodes - 1)
    def _():
        side = nbc[1]
        near([side[k : k + 1, :] for k in range(3)], nbw[1], False)

    def send_rows():
        await_bytes(asked, nodes - 1, recv_sem.at[1])
        spread = jnp.broadcast_to(asked[...], (nodes, CAP, 128))
        spread = jnp.where(iota(spread.shape, 2) == iota(spread.shape, 1), spread, 0.0)
        flat = jnp.sum(spread.reshape(slots, 128), axis=1, keepdims=True)
        hot[...] = jnp.where(flat == (iota((slots, leaf), 1) + 1).astype(F32), 1.0, 0.0).astype(BF16)
        rout[...] = dot(hot[...], omega_ref[...]).reshape(nodes, CAP, samp).astype(BF16)
        exchange(rout, rin, 3)

    def send_products():
        await_bytes(zin, planes - 1, recv_sem.at[6])
        points = jnp.concatenate([zin[i] for i in range(planes)], axis=1)
        points = jnp.concatenate([points, jnp.zeros((5, slots), F32)], axis=0)
        parts = jnp.concatenate(split3(points) + (jnp.zeros((8, slots), F32),), axis=0).astype(BF16)
        picked = dot(parts, scatter_hot[...])
        skel = picked[0:8] + picked[8:16] + picked[16:24]
        skel_rows = [skel[k : k + 1, :] for k in range(3)]
        for m in range(leaf // 128):
            part = pl.ds(m * 128, 128)
            columns = [jnp.concatenate([own_wide[k, part, :]] * (rank_size // 128), axis=1) for k in range(3)]
            tile[part, :] = kernel_tile(columns, skel_rows)
        transposed = dot(omega_t[...], tile[...]).astype(BF16)
        pout[...] = dot_nt(scatter_hot[...], transposed).reshape(nodes, CAP, samp).astype(BF16)
        exchange(pout, pin, 4)

    if ROWS_FIRST:
        send_rows()
        send_products()
    else:
        send_products()
        send_rows()
    spots[...] = jnp.transpose(hot[...])

    await_bytes(rin, nodes - 1, recv_sem.at[3])
    got = rin[...].astype(F32).reshape(slots, samp).astype(BF16)
    skel_samples = dot(gather_hot, got).astype(BF16)
    row_ref[...] = (acc[...] + dot(tile[...], skel_samples)).astype(BF16)

    await_bytes(lists, reps - 1, send_sem.at[0])
    await_bytes(line, LINE - 1, send_sem.at[5])
    for which, ref in ((1, reqs), (3, rout), (4, pout)):
        await_bytes(ref, nodes - 1, send_sem.at[which])
    for which, ref in ((2, zreq), (6, zout)):
        await_bytes(ref, planes - 1, send_sem.at[which])
    for copy in nb_copies:
        copy.wait_send()
    await_bytes(pin, nodes - 1, recv_sem.at[4])


def finish_kernel(row_ref, pin, spots, row_hbm, col_hbm, incoming, col_ref, sems):
    leaf = row_ref.shape[0]
    copies = [pltpu.make_async_copy(row_ref, row_hbm, sems.at[0])]
    copies[0].start()
    incoming[...] = pin[...].astype(F32).reshape(incoming.shape).astype(BF16)
    step = leaf // 2
    for k in range(2):
        part = pl.ds(k * step, step)
        col_ref[part, :] = dot(spots[part, :], incoming[...])
        copies.append(pltpu.make_async_copy(col_ref.at[part], col_hbm.at[part], sems.at[1 + k]))
        copies[-1].start()
    for copy in copies:
        copy.wait()


def solution(mesh):
    nodes, reps = mesh.shape["node"], mesh.shape["rep"]

    def on_device(coords, omega, skeleton):
        leaf, samp = omega.shape
        share = skeleton.shape[1]
        vmem = pl.BlockSpec(memory_space=pltpu.VMEM)
        anywhere = pl.BlockSpec(memory_space=pl.ANY)
        row, incoming, spots = pl.pallas_call(
            functools.partial(level_kernel, nodes, reps),
            out_shape=(
                jax.ShapeDtypeStruct((leaf, samp), BF16),
                jax.ShapeDtypeStruct((nodes, CAP, samp), BF16),
                jax.ShapeDtypeStruct((leaf, nodes * CAP), BF16),
            ),
            in_specs=[pl.BlockSpec(memory_space=pltpu.HBM)] * 3,
            out_specs=(vmem,) * 3,
            scratch_shapes=[
                pltpu.VMEM(coords.shape, F32),
                pltpu.VMEM((leaf, samp), BF16),
                pltpu.VMEM((1, share), jnp.int32),
                pltpu.VMEM((reps, 1, share), jnp.int32),
                pltpu.VMEM((nodes, 1, 128), F32),
                pltpu.VMEM((nodes, 1, 128), F32),
                pltpu.VMEM((nodes // LINE, 1, 128), F32),
                pltpu.VMEM((nodes // LINE, 1, 128), F32),
                pltpu.VMEM((nodes // LINE, 3, 128), F32),
                pltpu.VMEM((nodes // LINE, 3, 128), F32),
                pltpu.VMEM((LINE, 3, leaf), F32),
                pltpu.VMEM((nodes, CAP, samp), BF16),
                pltpu.VMEM((nodes, CAP, samp), BF16),
                pltpu.VMEM((nodes, CAP, samp), BF16),
                pltpu.VMEM((2, 3, leaf), F32),
                pltpu.VMEM((2, leaf, samp), BF16),
                pltpu.VMEM((leaf, 128), F32),
                pltpu.VMEM((3, leaf, 128), F32),
                pltpu.VMEM((samp, leaf), BF16),
                pltpu.VMEM((9 * LINE, leaf), BF16),
                pltpu.VMEM((leaf, samp), F32),
                pltpu.VMEM((nodes * CAP, leaf), BF16),
                pltpu.VMEM((nodes * CAP, share * reps), BF16),
                pltpu.VMEM((leaf, share * reps), BF16),
                pltpu.SemaphoreType.DMA((3,)),
                pltpu.SemaphoreType.REGULAR,
                pltpu.SemaphoreType.DMA((7,)),
                pltpu.SemaphoreType.DMA((7,)),
                pltpu.SemaphoreType.DMA((2, 2)),
                pltpu.SemaphoreType.DMA((2, 2)),
            ],
            compiler_params=pltpu.CompilerParams(
                collective_id=0, has_side_effects=True, vmem_limit_bytes=VMEM_LIMIT
            ),
        )(*(pltpu.with_memory_space_constraint(a, pltpu.HBM) for a in (coords, omega, skeleton)))
        return pl.pallas_call(
            finish_kernel,
            out_shape=(
                jax.ShapeDtypeStruct((leaf, samp), BF16),
                jax.ShapeDtypeStruct((leaf, samp), F32),
            ),
            in_specs=[vmem] * 3,
            out_specs=(anywhere,) * 2,
            scratch_shapes=[
                pltpu.VMEM((nodes * CAP, samp), BF16),
                pltpu.VMEM((leaf, samp), F32),
                pltpu.SemaphoreType.DMA((3,)),
            ],
            compiler_params=pltpu.CompilerParams(vmem_limit_bytes=VMEM_LIMIT),
        )(row, incoming, spots)

    return jax.shard_map(
        on_device,
        mesh=mesh,
        in_specs=(P(None, "node"), P("node", "rep"), P("node", "rep")),
        out_specs=(P("node", "rep"), P("node", "rep")),
        check_vma=False,
    )
```

```python
import functools

import jax
import jax.numpy as jnp
from jax import lax
from jax.experimental import pallas as pl
from jax.experimental.pallas import tpu as pltpu
from jax.sharding import PartitionSpec as P

MESH = pl.DeviceIdType.MESH
kernel_scale = 0.0078125
softening = 0.02
CAP = 8
LINE = 16
Y_ORDER = (8, 7, 9, 6, 10, 5, 11, 4, 12, 3, 13, 2, 14, 1, 15)
Z_ORDER = (4, 3, 5, 2, 6, 1, 7)
FAR = (4, 3, -3, 2, -2, 1, -1, 0)
REQUEST_ORDER = (0, 1, -1, 2, -2, 3, -3, 4)
ROW_ORDER = (0, 1, -1, 2, -2, 3, -3, 4)
VMEM_LIMIT = 24 << 20
F32 = jnp.float32
BF16 = jnp.bfloat16


def dot(a, b):
    return jnp.dot(a, b, preferred_element_type=F32)


def dot_tn(a, b):
    return lax.dot_general(a, b, (((0,), (0,)), ((), ())), preferred_element_type=F32)


def dot_nt(a, b):
    return lax.dot_general(a, b, (((1,), (1,)), ((), ())), preferred_element_type=F32)


def iota(shape, dim):
    return lax.broadcasted_iota(jnp.int32, shape, dim)


def kernel_tile(columns, rows):
    squared = (columns[0] - rows[0]) ** 2
    squared = squared + (columns[1] - rows[1]) ** 2
    squared = squared + (columns[2] - rows[2]) ** 2
    return (kernel_scale * lax.rsqrt(squared + softening * softening)).astype(BF16)


def split3(values):
    high = values.astype(BF16).astype(F32)
    rest = values - high
    middle = rest.astype(BF16).astype(F32)
    return high, middle, rest - middle


def far_first(rows, cols):
    def wrapped(value, size):
        return (value + size // 2 - 1) % size - (size // 2 - 1)

    seen, groups = {(0, 0)}, []
    for a in range(rows):
        for b in range(cols):
            group = []
            for p, q in ((a, b), (-b, a), (-a, -b), (b, -a)):
                pair = (wrapped(p, rows), wrapped(q, cols))
                if pair not in seen:
                    seen.add(pair)
                    group.append(pair)
            if group:
                groups.append(group)
    groups.sort(key=lambda g: -(abs(g[0][0]) + abs(g[0][1])))
    return [pair for group in groups for pair in group]


def level_kernel(
    nodes, reps, coords_hbm, omega_hbm, skel_hbm, row_ref, pin, spots,
    coords_ref, omega_ref, skel_ref, lists, reqs, asked, zreq, zasked, zout, zin, line, rout, rin, pout,
    nbc, nbw, own_t, own_wide, omega_t, table, acc, hot, scatter_hot, tile,
    gather_hot, load_sem, plane_sem, send_sem, recv_sem, asked_sem, nb_send, nb_recv,
):
    me, rep = lax.axis_index("node"), lax.axis_index("rep")
    leaf = coords_ref.shape[1]
    samp = omega_ref.shape[1]
    share = skel_ref.shape[1]
    rank_size = share * reps
    slots = nodes * CAP
    z, y, core = me // LINE, lax.rem(me // 2, LINE // 2), lax.rem(me, 2)
    spot = lax.rem(me, LINE)
    planes = nodes // LINE
    offsets = far_first(8, 8)

    def z_peer(d):
        return lax.rem(z + d, planes)

    def y_peer(d):
        return z * LINE + lax.rem(spot + d, LINE)

    barrier = pltpu.get_barrier_semaphore()

    loads = [
        pltpu.make_async_copy(src, dst, load_sem.at[k])
        for k, (src, dst) in enumerate(((skel_hbm, skel_ref), (coords_hbm, coords_ref), (omega_hbm, omega_ref)))
    ]
    for load in loads:
        load.start()

    def hello(node, column):
        pl.semaphore_signal(barrier, inc=1, device_id=(node, column), device_id_type=MESH)

    for d in Z_ORDER:
        hello(z_peer(d) * LINE + spot, rep)
    for d in Y_ORDER:
        hello(y_peer(d), rep)
    for d in range(1, reps):
        hello(me, lax.rem(rep + d, reps))

    loads[0].wait()
    loads[1].wait()
    pl.semaphore_wait(barrier, reps - 1 + LINE - 1 + planes - 1)

    for d in range(1, reps):
        pltpu.make_async_remote_copy(
            src_ref=skel_ref, dst_ref=lists.at[rep], send_sem=send_sem.at[0], recv_sem=recv_sem.at[0],
            device_id=(me, lax.rem(rep + d, reps)), device_id_type=MESH,
        ).start()
    for d in Z_ORDER:
        pl.semaphore_signal(plane_sem, inc=1, device_id=(z_peer(d) * LINE + spot, rep), device_id_type=MESH)
    for d in Y_ORDER:
        pltpu.make_async_remote_copy(
            src_ref=coords_ref, dst_ref=line.at[spot], send_sem=send_sem.at[5], recv_sem=recv_sem.at[5],
            device_id=(y_peer(d), rep), device_id_type=MESH,
        ).start()

    loads[2].wait()
    lists[rep] = skel_ref[...]
    line[spot] = coords_ref[...]
    asked[me] = jnp.zeros((1, 128), F32)
    rin[me] = jnp.zeros((CAP, samp), BF16)
    pin[me] = jnp.zeros((CAP, samp), BF16)
    own = coords_ref[...]
    own_rows = [own[k : k + 1, :] for k in range(3)]
    own_t[...] = jnp.transpose(jnp.concatenate([own, jnp.zeros((128 - 3, leaf), F32)], axis=0))
    for k in range(3):
        own_wide[k] = jnp.broadcast_to(own_t[:, k : k + 1], (leaf, 128))

    def near(point_rows, sample_rows, first):
        @pl.loop(0, leaf // 128)
        def _(m):
            part = pl.ds(pl.multiple_of(m * 128, 128), 128)
            columns = [jnp.concatenate([own_wide[k, part, :]] * (leaf // 128), axis=1) for k in range(3)]
            term = dot(kernel_tile(columns, point_rows), sample_rows)
            acc[part, :] = term if first else acc[part, :] + term

    near(own_rows, omega_ref[...], True)

    nb_copies = []
    for side, step in ((0, 1), (1, nodes - 1)):
        for j, (src, dst) in enumerate(((coords_ref, nbc), (omega_ref, nbw))):
            nb_copies.append(
                pltpu.make_async_remote_copy(
                    src_ref=src, dst_ref=dst.at[side], send_sem=nb_send.at[side, j], recv_sem=nb_recv.at[side, j],
                    device_id=(lax.rem(me + step, nodes), rep), device_id_type=MESH,
                )
            )

    def await_bytes(ref, count, sem):
        view = ref.at[pl.ds(0, count)]
        pltpu.make_async_copy(view, view, sem).wait()

    def send_to(src, dst, target, out_sem, in_sem):
        pltpu.make_async_remote_copy(
            src_ref=src.at[target], dst_ref=dst.at[me], send_sem=out_sem, recv_sem=in_sem,
            device_id=(target, rep), device_id_type=MESH,
        ).start()

    def send_pair(src, dst, chip, out_sem, in_sem, own_chip):
        if not own_chip:
            send_to(src, dst, chip + core, out_sem, in_sem)
        send_to(src, dst, chip + 1 - core, out_sem, in_sem)

    def exchange(src, dst, which):
        for dy, dz in offsets + [(0, 0)]:
            chip = lax.rem(z + (dz + 8), 8) * LINE + lax.rem(y + (dy + 8), 8) * 2
            send_pair(src, dst, chip, send_sem.at[which], recv_sem.at[which], dy == 0 and dz == 0)

    def z_exchange(src, dst, which):
        for d in Z_ORDER:
            pltpu.make_async_remote_copy(
                src_ref=src.at[z_peer(d)], dst_ref=dst.at[z], send_sem=send_sem.at[which], recv_sem=recv_sem.at[which],
                device_id=(z_peer(d) * LINE + spot, rep), device_id_type=MESH,
            ).start()

    await_bytes(lists, reps - 1, recv_sem.at[0])

    listed = jnp.concatenate([lists[r] for r in range(reps)], axis=1)
    owner_row = listed >> 9
    listed_col = jnp.transpose(jnp.broadcast_to(listed.astype(F32), (128, rank_size))).astype(jnp.int32)
    owner_col = listed_col >> 9
    value_col = (listed_col & (leaf - 1)) + 1
    wide_owner = jnp.concatenate([owner_col] * (rank_size // 128), axis=1)
    same = wide_owner == owner_row
    before = jnp.where(same & (iota(same.shape, 1) < iota(same.shape, 0)), 1.0, 0.0).astype(BF16)
    rank_col = dot(before, jnp.ones((rank_size, 128), BF16)).astype(jnp.int32)
    low_col = (value_col & 255).astype(F32)
    high_col = (value_col >> 8).astype(F32)

    def requests(lane_col, owner_hot):
        placed = lane_col == iota((rank_size, 128), 1)
        low = jnp.where(placed, low_col, 0.0).astype(BF16)
        high = jnp.where(placed, high_col, 0.0).astype(BF16)
        return dot(owner_hot, low) + 256.0 * dot(owner_hot, high)

    z_hot = jnp.where((owner_row >> 4) == iota((16, rank_size), 0), 1.0, 0.0).astype(BF16)
    z_request = requests((owner_col & (LINE - 1)) * CAP + rank_col, z_hot)
    for i in range(planes):
        zreq[i] = z_request[i : i + 1, :]
    z_exchange(zreq, zasked, 2)
    zasked[z] = zreq[z]

    owner_hot = jnp.where(owner_row == iota((nodes, rank_size), 0), 1.0, 0.0).astype(BF16)
    reqs[...] = requests(rank_col, owner_hot).reshape(nodes, 1, 128)
    pl.semaphore_wait(plane_sem, planes - 1)
    for dz in REQUEST_ORDER:
        base = z_peer(planes + dz) * LINE
        for dy in FAR:
            chip = base + lax.rem(y + (dy + 8), 8) * 2
            send_pair(reqs, asked, chip, send_sem.at[1], asked_sem.at[z], dy == 0 and dz == 0)
    for copy in nb_copies:
        copy.start()

    await_bytes(line, LINE - 1, recv_sem.at[5])
    for k in range(3):
        for part, values in enumerate(split3(jnp.concatenate([line[n, k : k + 1, :] for n in range(LINE)], axis=0))):
            table[pl.ds((3 * k + part) * LINE, LINE), :] = values.astype(BF16)

    flat_col = owner_col * CAP + rank_col
    flat_wide = jnp.concatenate([flat_col] * (slots // 128), axis=1)
    gather_hot[...] = jnp.where(flat_wide == iota((rank_size, slots), 1), 1.0, 0.0).astype(BF16)
    earlier = jnp.where(same & (iota(same.shape, 0) < iota(same.shape, 1)), 1.0, 0.0)
    rank_row = jnp.sum(earlier, axis=0, keepdims=True).astype(jnp.int32)
    flat_row = owner_row * CAP + rank_row
    scatter_hot[...] = jnp.where(flat_row == iota((slots, rank_size), 0), 1.0, 0.0).astype(BF16)

    omega_t[...] = jnp.transpose(omega_ref[...])

    await_bytes(zasked, planes - 1, recv_sem.at[2])
    width = 256
    for c in range(slots // width):
        wanted = jnp.concatenate([zasked[2 * c], zasked[2 * c + 1]], axis=1)
        point_hot = jnp.where(wanted == (iota((leaf, width), 0) + 1).astype(F32), 1.0, 0.0).astype(BF16)
        found = dot(table[...], point_hot)
        own_node = lax.rem(iota((3 * LINE, width), 0), LINE) == lax.rem(iota((3 * LINE, width), 1) // CAP, LINE)
        answer = jnp.concatenate(
            [
                jnp.sum(jnp.where(own_node, found[3 * LINE * k : 3 * LINE * (k + 1)], 0.0), axis=0, keepdims=True)
                for k in range(3)
            ],
            axis=0,
        )
        zout[2 * c] = answer[:, :128]
        zout[2 * c + 1] = answer[:, 128:]
    z_exchange(zout, zin, 6)
    zin[z] = zout[z]

    point = (iota((LINE * CAP, leaf), 1) + 1).astype(F32)
    for dz in ROW_ORDER:
        zs = z_peer(planes + dz)
        nodes_of = pl.ds(pl.multiple_of(zs * LINE, LINE), LINE)
        slots_of = pl.ds(pl.multiple_of(zs * LINE * CAP, LINE * CAP), LINE * CAP)
        await_bytes(asked, LINE if dz else LINE - 1, asked_sem.at[zs])
        spread = jnp.broadcast_to(asked[nodes_of], (LINE, CAP, 128))
        spread = jnp.where(iota(spread.shape, 2) == iota(spread.shape, 1), spread, 0.0)
        flat = jnp.sum(spread.reshape(LINE * CAP, 128), axis=1, keepdims=True)
        point_hot = jnp.where(flat == point, 1.0, 0.0).astype(BF16)
        hot[slots_of, :] = point_hot
        rout[nodes_of] = dot(point_hot, omega_ref[...]).reshape(LINE, CAP, samp).astype(BF16)
        for dy in FAR:
            chip = zs * LINE + lax.rem(y + (dy + 8), 8) * 2
            send_pair(rout, rin, chip, send_sem.at[3], recv_sem.at[3], dy == 0 and dz == 0)

    def send_products():
        await_bytes(zin, planes - 1, recv_sem.at[6])
        points = jnp.concatenate([zin[i] for i in range(planes)], axis=1)
        points = jnp.concatenate([points, jnp.zeros((5, slots), F32)], axis=0)
        parts = jnp.concatenate(split3(points) + (jnp.zeros((8, slots), F32),), axis=0).astype(BF16)
        picked = dot(parts, scatter_hot[...])
        skel = picked[0:8] + picked[8:16] + picked[16:24]
        skel_rows = [skel[k : k + 1, :] for k in range(3)]
        for m in range(leaf // 128):
            part = pl.ds(m * 128, 128)
            columns = [jnp.concatenate([own_wide[k, part, :]] * (rank_size // 128), axis=1) for k in range(3)]
            tile[part, :] = kernel_tile(columns, skel_rows)
        transposed = dot(omega_t[...], tile[...]).astype(BF16)
        pout[...] = dot_nt(scatter_hot[...], transposed).reshape(nodes, CAP, samp).astype(BF16)
        exchange(pout, pin, 4)

    send_products()

    for copy in nb_copies:
        copy.wait_recv()

    @pl.when(me > 0)
    def _():
        side = nbc[0]
        near([side[k : k + 1, :] for k in range(3)], nbw[0], False)

    @pl.when(me < nodes - 1)
    def _():
        side = nbc[1]
        near([side[k : k + 1, :] for k in range(3)], nbw[1], False)

    spots[...] = jnp.transpose(hot[...])

    await_bytes(rin, nodes - 1, recv_sem.at[3])
    got = rin[...].astype(F32).reshape(slots, samp).astype(BF16)
    skel_samples = dot(gather_hot[...], got).astype(BF16)
    row_ref[...] = (acc[...] + dot(tile[...], skel_samples)).astype(BF16)

    await_bytes(lists, reps - 1, send_sem.at[0])
    await_bytes(line, LINE - 1, send_sem.at[5])
    for which, ref in ((1, reqs), (3, rout), (4, pout)):
        await_bytes(ref, nodes - 1, send_sem.at[which])
    for which, ref in ((2, zreq), (6, zout)):
        await_bytes(ref, planes - 1, send_sem.at[which])
    for copy in nb_copies:
        copy.wait_send()
    await_bytes(pin, nodes - 1, recv_sem.at[4])


def finish_kernel(row_ref, pin, spots, row_hbm, col_hbm, incoming, col_ref, sems):
    leaf = row_ref.shape[0]
    copies = [pltpu.make_async_copy(row_ref, row_hbm, sems.at[0])]
    copies[0].start()
    incoming[...] = pin[...].astype(F32).reshape(incoming.shape).astype(BF16)
    step = leaf // 2
    for k in range(2):
        part = pl.ds(k * step, step)
        col_ref[part, :] = dot(spots[part, :], incoming[...])
        copies.append(pltpu.make_async_copy(col_ref.at[part], col_hbm.at[part], sems.at[1 + k]))
        copies[-1].start()
    for copy in copies:
        copy.wait()


def solution(mesh):
    nodes, reps = mesh.shape["node"], mesh.shape["rep"]

    def on_device(coords, omega, skeleton):
        leaf, samp = omega.shape
        share = skeleton.shape[1]
        vmem = pl.BlockSpec(memory_space=pltpu.VMEM)
        anywhere = pl.BlockSpec(memory_space=pl.ANY)
        row, incoming, spots = pl.pallas_call(
            functools.partial(level_kernel, nodes, reps),
            out_shape=(
                jax.ShapeDtypeStruct((leaf, samp), BF16),
                jax.ShapeDtypeStruct((nodes, CAP, samp), BF16),
                jax.ShapeDtypeStruct((leaf, nodes * CAP), BF16),
            ),
            in_specs=[pl.BlockSpec(memory_space=pltpu.HBM)] * 3,
            out_specs=(vmem,) * 3,
            scratch_shapes=[
                pltpu.VMEM(coords.shape, F32),
                pltpu.VMEM((leaf, samp), BF16),
                pltpu.VMEM((1, share), jnp.int32),
                pltpu.VMEM((reps, 1, share), jnp.int32),
                pltpu.VMEM((nodes, 1, 128), F32),
                pltpu.VMEM((nodes, 1, 128), F32),
                pltpu.VMEM((nodes // LINE, 1, 128), F32),
                pltpu.VMEM((nodes // LINE, 1, 128), F32),
                pltpu.VMEM((nodes // LINE, 3, 128), F32),
                pltpu.VMEM((nodes // LINE, 3, 128), F32),
                pltpu.VMEM((LINE, 3, leaf), F32),
                pltpu.VMEM((nodes, CAP, samp), BF16),
                pltpu.VMEM((nodes, CAP, samp), BF16),
                pltpu.VMEM((nodes, CAP, samp), BF16),
                pltpu.VMEM((2, 3, leaf), F32),
                pltpu.VMEM((2, leaf, samp), BF16),
                pltpu.VMEM((leaf, 128), F32),
                pltpu.VMEM((3, leaf, 128), F32),
                pltpu.VMEM((samp, leaf), BF16),
                pltpu.VMEM((9 * LINE, leaf), BF16),
                pltpu.VMEM((leaf, samp), F32),
                pltpu.VMEM((nodes * CAP, leaf), BF16),
                pltpu.VMEM((nodes * CAP, share * reps), BF16),
                pltpu.VMEM((leaf, share * reps), BF16),
                pltpu.VMEM((share * reps, nodes * CAP), BF16),
                pltpu.SemaphoreType.DMA((3,)),
                pltpu.SemaphoreType.REGULAR,
                pltpu.SemaphoreType.DMA((7,)),
                pltpu.SemaphoreType.DMA((7,)),
                pltpu.SemaphoreType.DMA((nodes // LINE,)),
                pltpu.SemaphoreType.DMA((2, 2)),
                pltpu.SemaphoreType.DMA((2, 2)),
            ],
            compiler_params=pltpu.CompilerParams(
                collective_id=0, has_side_effects=True, vmem_limit_bytes=VMEM_LIMIT
            ),
        )(*(pltpu.with_memory_space_constraint(a, pltpu.HBM) for a in (coords, omega, skeleton)))
        return pl.pallas_call(
            finish_kernel,
            out_shape=(
                jax.ShapeDtypeStruct((leaf, samp), BF16),
                jax.ShapeDtypeStruct((leaf, samp), F32),
            ),
            in_specs=[vmem] * 3,
            out_specs=(anywhere,) * 2,
            scratch_shapes=[
                pltpu.VMEM((nodes * CAP, samp), BF16),
                pltpu.VMEM((leaf, samp), F32),
                pltpu.SemaphoreType.DMA((3,)),
            ],
            compiler_params=pltpu.CompilerParams(vmem_limit_bytes=VMEM_LIMIT),
        )(row, incoming, spots)

    return jax.shard_map(
        on_device,
        mesh=mesh,
        in_specs=(P(None, "node"), P("node", "rep"), P("node", "rep")),
        out_specs=(P("node", "rep"), P("node", "rep")),
        check_vma=False,
    )
```

```python
import functools

import jax
import jax.numpy as jnp
from jax import lax
from jax.experimental import pallas as pl
from jax.experimental.pallas import tpu as pltpu
from jax.sharding import PartitionSpec as P

MESH = pl.DeviceIdType.MESH
kernel_scale = 0.0078125
softening = 0.02
CAP = 8
LINE = 16
Y_ORDER = (8, 7, 9, 6, 10, 5, 11, 4, 12, 3, 13, 2, 14, 1, 15)
Z_ORDER = (4, 3, 5, 2, 6, 1, 7)
FAR = (4, 3, -3, 2, -2, 1, -1, 0)
REQUEST_ORDER = (0, 1, -1, 2, -2, 3, -3, 4)
ROW_ORDER = (0, 1, -1, 2, -2, 3, -3, 4)
VMEM_LIMIT = 24 << 20
F32 = jnp.float32
BF16 = jnp.bfloat16


def dot(a, b):
    return jnp.dot(a, b, preferred_element_type=F32)


def dot_tn(a, b):
    return lax.dot_general(a, b, (((0,), (0,)), ((), ())), preferred_element_type=F32)


def dot_nt(a, b):
    return lax.dot_general(a, b, (((1,), (1,)), ((), ())), preferred_element_type=F32)


def iota(shape, dim):
    return lax.broadcasted_iota(jnp.int32, shape, dim)


def kernel_tile(columns, rows):
    squared = (columns[0] - rows[0]) ** 2
    squared = squared + (columns[1] - rows[1]) ** 2
    squared = squared + (columns[2] - rows[2]) ** 2
    return (kernel_scale * lax.rsqrt(squared + softening * softening)).astype(BF16)


def split3(values):
    high = values.astype(BF16).astype(F32)
    rest = values - high
    middle = rest.astype(BF16).astype(F32)
    return high, middle, rest - middle


def far_first(rows, cols):
    def wrapped(value, size):
        return (value + size // 2 - 1) % size - (size // 2 - 1)

    seen, groups = {(0, 0)}, []
    for a in range(rows):
        for b in range(cols):
            group = []
            for p, q in ((a, b), (-b, a), (-a, -b), (b, -a)):
                pair = (wrapped(p, rows), wrapped(q, cols))
                if pair not in seen:
                    seen.add(pair)
                    group.append(pair)
            if group:
                groups.append(group)
    groups.sort(key=lambda g: -(abs(g[0][0]) + abs(g[0][1])))
    flat = [pair for group in groups for pair in group]
    return sorted(flat, key=lambda p: -(2 * abs(p[0]) + abs(p[1])))


def level_kernel(
    nodes, reps, coords_hbm, omega_hbm, skel_hbm, row_ref, pin, spots,
    coords_ref, omega_ref, skel_ref, lists, reqs, asked, zreq, zasked, zout, zin, line, rout, rin, pout,
    nbc, nbw, own_t, own_wide, omega_t, table, acc, hot, scatter_hot, tile,
    gather_hot, load_sem, plane_sem, send_sem, recv_sem, asked_sem, nb_send, nb_recv,
):
    me, rep = lax.axis_index("node"), lax.axis_index("rep")
    leaf = coords_ref.shape[1]
    samp = omega_ref.shape[1]
    share = skel_ref.shape[1]
    rank_size = share * reps
    slots = nodes * CAP
    z, y, core = me // LINE, lax.rem(me // 2, LINE // 2), lax.rem(me, 2)
    spot = lax.rem(me, LINE)
    planes = nodes // LINE
    offsets = far_first(8, 8)

    def z_peer(d):
        return lax.rem(z + d, planes)

    def y_peer(d):
        return z * LINE + lax.rem(spot + d, LINE)

    barrier = pltpu.get_barrier_semaphore()

    loads = [
        pltpu.make_async_copy(src, dst, load_sem.at[k])
        for k, (src, dst) in enumerate(((skel_hbm, skel_ref), (coords_hbm, coords_ref), (omega_hbm, omega_ref)))
    ]
    for load in loads:
        load.start()

    def hello(node, column):
        pl.semaphore_signal(barrier, inc=1, device_id=(node, column), device_id_type=MESH)

    for d in Z_ORDER:
        hello(z_peer(d) * LINE + spot, rep)
    for d in Y_ORDER:
        hello(y_peer(d), rep)
    for d in range(1, reps):
        hello(me, lax.rem(rep + d, reps))
    for d in (1, nodes - 1):
        hello(lax.rem(me + d, nodes), rep)

    loads[0].wait()
    loads[1].wait()
    pl.semaphore_wait(barrier, reps - 1 + LINE - 1 + planes - 1 + 2)

    for d in range(1, reps):
        pltpu.make_async_remote_copy(
            src_ref=skel_ref, dst_ref=lists.at[rep], send_sem=send_sem.at[0], recv_sem=recv_sem.at[0],
            device_id=(me, lax.rem(rep + d, reps)), device_id_type=MESH,
        ).start()
    for d in Z_ORDER:
        pl.semaphore_signal(plane_sem, inc=1, device_id=(z_peer(d) * LINE + spot, rep), device_id_type=MESH)
    for d in Y_ORDER:
        pltpu.make_async_remote_copy(
            src_ref=coords_ref, dst_ref=line.at[spot], send_sem=send_sem.at[5], recv_sem=recv_sem.at[5],
            device_id=(y_peer(d), rep), device_id_type=MESH,
        ).start()

    nb_copies = []
    for side, step in ((0, 1), (1, nodes - 1)):
        for j, (src, dst) in enumerate(((coords_ref, nbc), (omega_ref, nbw))):
            nb_copies.append(
                pltpu.make_async_remote_copy(
                    src_ref=src, dst_ref=dst.at[side], send_sem=nb_send.at[side, j], recv_sem=nb_recv.at[side, j],
                    device_id=(lax.rem(me + step, nodes), rep), device_id_type=MESH,
                )
            )
    loads[2].wait()
    for copy in nb_copies:
        copy.start()

    lists[rep] = skel_ref[...]
    line[spot] = coords_ref[...]
    asked[me] = jnp.zeros((1, 128), F32)
    rin[me] = jnp.zeros((CAP, samp), BF16)
    pin[me] = jnp.zeros((CAP, samp), BF16)
    own = coords_ref[...]
    own_rows = [own[k : k + 1, :] for k in range(3)]
    own_t[...] = jnp.transpose(jnp.concatenate([own, jnp.zeros((128 - 3, leaf), F32)], axis=0))
    for k in range(3):
        own_wide[k] = jnp.broadcast_to(own_t[:, k : k + 1], (leaf, 128))

    def near(point_rows, sample_rows, first):
        @pl.loop(0, leaf // 128)
        def _(m):
            part = pl.ds(pl.multiple_of(m * 128, 128), 128)
            columns = [jnp.concatenate([own_wide[k, part, :]] * (leaf // 128), axis=1) for k in range(3)]
            term = dot(kernel_tile(columns, point_rows), sample_rows)
            acc[part, :] = term if first else acc[part, :] + term

    near(own_rows, omega_ref[...], True)

    def await_bytes(ref, count, sem):
        view = ref.at[pl.ds(0, count)]
        pltpu.make_async_copy(view, view, sem).wait()

    def send_to(src, dst, target, out_sem, in_sem):
        pltpu.make_async_remote_copy(
            src_ref=src.at[target], dst_ref=dst.at[me], send_sem=out_sem, recv_sem=in_sem,
            device_id=(target, rep), device_id_type=MESH,
        ).start()

    def send_pair(src, dst, chip, out_sem, in_sem, own_chip):
        if not own_chip:
            send_to(src, dst, chip + core, out_sem, in_sem)
        send_to(src, dst, chip + 1 - core, out_sem, in_sem)

    def exchange(src, dst, which):
        for dy, dz in offsets + [(0, 0)]:
            chip = lax.rem(z + (dz + 8), 8) * LINE + lax.rem(y + (dy + 8), 8) * 2
            send_pair(src, dst, chip, send_sem.at[which], recv_sem.at[which], dy == 0 and dz == 0)

    def z_exchange(src, dst, which):
        for d in Z_ORDER:
            pltpu.make_async_remote_copy(
                src_ref=src.at[z_peer(d)], dst_ref=dst.at[z], send_sem=send_sem.at[which], recv_sem=recv_sem.at[which],
                device_id=(z_peer(d) * LINE + spot, rep), device_id_type=MESH,
            ).start()

    await_bytes(lists, reps - 1, recv_sem.at[0])

    listed = jnp.concatenate([lists[r] for r in range(reps)], axis=1)
    owner_row = listed >> 9
    listed_col = jnp.transpose(jnp.broadcast_to(listed.astype(F32), (128, rank_size))).astype(jnp.int32)
    owner_col = listed_col >> 9
    value_col = (listed_col & (leaf - 1)) + 1
    wide_owner = jnp.concatenate([owner_col] * (rank_size // 128), axis=1)
    same = wide_owner == owner_row
    before = jnp.where(same & (iota(same.shape, 1) < iota(same.shape, 0)), 1.0, 0.0).astype(BF16)
    rank_col = dot(before, jnp.ones((rank_size, 128), BF16)).astype(jnp.int32)
    low_col = (value_col & 255).astype(F32)
    high_col = (value_col >> 8).astype(F32)

    def requests(lane_col, owner_hot):
        placed = lane_col == iota((rank_size, 128), 1)
        low = jnp.where(placed, low_col, 0.0).astype(BF16)
        high = jnp.where(placed, high_col, 0.0).astype(BF16)
        return dot(owner_hot, low) + 256.0 * dot(owner_hot, high)

    z_hot = jnp.where((owner_row >> 4) == iota((16, rank_size), 0), 1.0, 0.0).astype(BF16)
    z_request = requests((owner_col & (LINE - 1)) * CAP + rank_col, z_hot)
    for i in range(planes):
        zreq[i] = z_request[i : i + 1, :]
    z_exchange(zreq, zasked, 2)
    zasked[z] = zreq[z]

    owner_hot = jnp.where(owner_row == iota((nodes, rank_size), 0), 1.0, 0.0).astype(BF16)
    reqs[...] = requests(rank_col, owner_hot).reshape(nodes, 1, 128)
    pl.semaphore_wait(plane_sem, planes - 1)
    for dz in REQUEST_ORDER:
        base = z_peer(planes + dz) * LINE
        for dy in FAR:
            chip = base + lax.rem(y + (dy + 8), 8) * 2
            send_pair(reqs, asked, chip, send_sem.at[1], asked_sem.at[z], dy == 0 and dz == 0)

    await_bytes(line, LINE - 1, recv_sem.at[5])
    for k in range(3):
        for part, values in enumerate(split3(jnp.concatenate([line[n, k : k + 1, :] for n in range(LINE)], axis=0))):
            table[pl.ds((3 * k + part) * LINE, LINE), :] = values.astype(BF16)

    flat_col = owner_col * CAP + rank_col
    flat_wide = jnp.concatenate([flat_col] * (slots // 128), axis=1)
    gather_hot[...] = jnp.where(flat_wide == iota((rank_size, slots), 1), 1.0, 0.0).astype(BF16)
    earlier = jnp.where(same & (iota(same.shape, 0) < iota(same.shape, 1)), 1.0, 0.0)
    rank_row = jnp.sum(earlier, axis=0, keepdims=True).astype(jnp.int32)
    flat_row = owner_row * CAP + rank_row
    scatter_hot[...] = jnp.where(flat_row == iota((slots, rank_size), 0), 1.0, 0.0).astype(BF16)

    omega_t[...] = jnp.transpose(omega_ref[...])

    await_bytes(zasked, planes - 1, recv_sem.at[2])
    width = 256
    for c in range(slots // width):
        wanted = jnp.concatenate([zasked[2 * c], zasked[2 * c + 1]], axis=1)
        point_hot = jnp.where(wanted == (iota((leaf, width), 0) + 1).astype(F32), 1.0, 0.0).astype(BF16)
        found = dot(table[...], point_hot)
        own_node = lax.rem(iota((3 * LINE, width), 0), LINE) == lax.rem(iota((3 * LINE, width), 1) // CAP, LINE)
        answer = jnp.concatenate(
            [
                jnp.sum(jnp.where(own_node, found[3 * LINE * k : 3 * LINE * (k + 1)], 0.0), axis=0, keepdims=True)
                for k in range(3)
            ],
            axis=0,
        )
        zout[2 * c] = answer[:, :128]
        zout[2 * c + 1] = answer[:, 128:]
    z_exchange(zout, zin, 6)
    zin[z] = zout[z]

    point = (iota((LINE * CAP, leaf), 1) + 1).astype(F32)
    for dz in ROW_ORDER:
        zs = z_peer(planes + dz)
        nodes_of = pl.ds(pl.multiple_of(zs * LINE, LINE), LINE)
        slots_of = pl.ds(pl.multiple_of(zs * LINE * CAP, LINE * CAP), LINE * CAP)
        await_bytes(asked, LINE if dz else LINE - 1, asked_sem.at[zs])
        spread = jnp.broadcast_to(asked[nodes_of], (LINE, CAP, 128))
        spread = jnp.where(iota(spread.shape, 2) == iota(spread.shape, 1), spread, 0.0)
        flat = jnp.sum(spread.reshape(LINE * CAP, 128), axis=1, keepdims=True)
        point_hot = jnp.where(flat == point, 1.0, 0.0).astype(BF16)
        hot[slots_of, :] = point_hot
        rout[nodes_of] = dot(point_hot, omega_ref[...]).reshape(LINE, CAP, samp).astype(BF16)
        for dy in FAR:
            chip = zs * LINE + lax.rem(y + (dy + 8), 8) * 2
            send_pair(rout, rin, chip, send_sem.at[3], recv_sem.at[3], dy == 0 and dz == 0)

    def send_products():
        await_bytes(zin, planes - 1, recv_sem.at[6])
        points = jnp.concatenate([zin[i] for i in range(planes)], axis=1)
        points = jnp.concatenate([points, jnp.zeros((5, slots), F32)], axis=0)
        parts = jnp.concatenate(split3(points) + (jnp.zeros((8, slots), F32),), axis=0).astype(BF16)
        picked = dot(parts, scatter_hot[...])
        skel = picked[0:8] + picked[8:16] + picked[16:24]
        skel_rows = [skel[k : k + 1, :] for k in range(3)]
        for m in range(leaf // 128):
            part = pl.ds(m * 128, 128)
            columns = [jnp.concatenate([own_wide[k, part, :]] * (rank_size // 128), axis=1) for k in range(3)]
            tile[part, :] = kernel_tile(columns, skel_rows)
        transposed = dot(omega_t[...], tile[...]).astype(BF16)
        pout[...] = dot_nt(scatter_hot[...], transposed).reshape(nodes, CAP, samp).astype(BF16)
        exchange(pout, pin, 4)

    send_products()

    for copy in nb_copies:
        copy.wait_recv()

    @pl.when(me > 0)
    def _():
        side = nbc[0]
        near([side[k : k + 1, :] for k in range(3)], nbw[0], False)

    @pl.when(me < nodes - 1)
    def _():
        side = nbc[1]
        near([side[k : k + 1, :] for k in range(3)], nbw[1], False)

    spots[...] = jnp.transpose(hot[...])

    await_bytes(rin, nodes - 1, recv_sem.at[3])
    got = rin[...].astype(F32).reshape(slots, samp).astype(BF16)
    skel_samples = dot(gather_hot[...], got).astype(BF16)
    row_ref[...] = (acc[...] + dot(tile[...], skel_samples)).astype(BF16)

    await_bytes(lists, reps - 1, send_sem.at[0])
    await_bytes(line, LINE - 1, send_sem.at[5])
    for which, ref in ((1, reqs), (3, rout), (4, pout)):
        await_bytes(ref, nodes - 1, send_sem.at[which])
    for which, ref in ((2, zreq), (6, zout)):
        await_bytes(ref, planes - 1, send_sem.at[which])
    for copy in nb_copies:
        copy.wait_send()
    await_bytes(pin, nodes - 1, recv_sem.at[4])


def finish_kernel(row_ref, pin, spots, row_hbm, col_hbm, incoming, col_ref, sems):
    leaf = row_ref.shape[0]
    copies = [pltpu.make_async_copy(row_ref, row_hbm, sems.at[0])]
    copies[0].start()
    incoming[...] = pin[...].astype(F32).reshape(incoming.shape).astype(BF16)
    step = leaf // 2
    for k in range(2):
        part = pl.ds(k * step, step)
        col_ref[part, :] = dot(spots[part, :], incoming[...])
        copies.append(pltpu.make_async_copy(col_ref.at[part], col_hbm.at[part], sems.at[1 + k]))
        copies[-1].start()
    for copy in copies:
        copy.wait()


def solution(mesh):
    nodes, reps = mesh.shape["node"], mesh.shape["rep"]

    def on_device(coords, omega, skeleton):
        leaf, samp = omega.shape
        share = skeleton.shape[1]
        vmem = pl.BlockSpec(memory_space=pltpu.VMEM)
        anywhere = pl.BlockSpec(memory_space=pl.ANY)
        row, incoming, spots = pl.pallas_call(
            functools.partial(level_kernel, nodes, reps),
            out_shape=(
                jax.ShapeDtypeStruct((leaf, samp), BF16),
                jax.ShapeDtypeStruct((nodes, CAP, samp), BF16),
                jax.ShapeDtypeStruct((leaf, nodes * CAP), BF16),
            ),
            in_specs=[pl.BlockSpec(memory_space=pltpu.HBM)] * 3,
            out_specs=(vmem,) * 3,
            scratch_shapes=[
                pltpu.VMEM(coords.shape, F32),
                pltpu.VMEM((leaf, samp), BF16),
                pltpu.VMEM((1, share), jnp.int32),
                pltpu.VMEM((reps, 1, share), jnp.int32),
                pltpu.VMEM((nodes, 1, 128), F32),
                pltpu.VMEM((nodes, 1, 128), F32),
                pltpu.VMEM((nodes // LINE, 1, 128), F32),
                pltpu.VMEM((nodes // LINE, 1, 128), F32),
                pltpu.VMEM((nodes // LINE, 3, 128), F32),
                pltpu.VMEM((nodes // LINE, 3, 128), F32),
                pltpu.VMEM((LINE, 3, leaf), F32),
                pltpu.VMEM((nodes, CAP, samp), BF16),
                pltpu.VMEM((nodes, CAP, samp), BF16),
                pltpu.VMEM((nodes, CAP, samp), BF16),
                pltpu.VMEM((2, 3, leaf), F32),
                pltpu.VMEM((2, leaf, samp), BF16),
                pltpu.VMEM((leaf, 128), F32),
                pltpu.VMEM((3, leaf, 128), F32),
                pltpu.VMEM((samp, leaf), BF16),
                pltpu.VMEM((9 * LINE, leaf), BF16),
                pltpu.VMEM((leaf, samp), F32),
                pltpu.VMEM((nodes * CAP, leaf), BF16),
                pltpu.VMEM((nodes * CAP, share * reps), BF16),
                pltpu.VMEM((leaf, share * reps), BF16),
                pltpu.VMEM((share * reps, nodes * CAP), BF16),
                pltpu.SemaphoreType.DMA((3,)),
                pltpu.SemaphoreType.REGULAR,
                pltpu.SemaphoreType.DMA((7,)),
                pltpu.SemaphoreType.DMA((7,)),
                pltpu.SemaphoreType.DMA((nodes // LINE,)),
                pltpu.SemaphoreType.DMA((2, 2)),
                pltpu.SemaphoreType.DMA((2, 2)),
            ],
            compiler_params=pltpu.CompilerParams(
                collective_id=0, has_side_effects=True, vmem_limit_bytes=VMEM_LIMIT
            ),
        )(*(pltpu.with_memory_space_constraint(a, pltpu.HBM) for a in (coords, omega, skeleton)))
        return pl.pallas_call(
            finish_kernel,
            out_shape=(
                jax.ShapeDtypeStruct((leaf, samp), BF16),
                jax.ShapeDtypeStruct((leaf, samp), F32),
            ),
            in_specs=[vmem] * 3,
            out_specs=(anywhere,) * 2,
            scratch_shapes=[
                pltpu.VMEM((nodes * CAP, samp), BF16),
                pltpu.VMEM((leaf, samp), F32),
                pltpu.SemaphoreType.DMA((3,)),
            ],
            compiler_params=pltpu.CompilerParams(vmem_limit_bytes=VMEM_LIMIT),
        )(row, incoming, spots)

    return jax.shard_map(
        on_device,
        mesh=mesh,
        in_specs=(P(None, "node"), P("node", "rep"), P("node", "rep")),
        out_specs=(P("node", "rep"), P("node", "rep")),
        check_vma=False,
    )
```

```python
import functools

import jax
import jax.numpy as jnp
from jax import lax
from jax.experimental import pallas as pl
from jax.experimental.pallas import tpu as pltpu
from jax.sharding import PartitionSpec as P

MESH = pl.DeviceIdType.MESH
kernel_scale = 0.0078125
softening = 0.02
CAP = 8
LINE = 16
Y_ORDER = (8, 7, 9, 6, 10, 5, 11, 4, 12, 3, 13, 2, 14, 1, 15)
Z_ORDER = (4, 3, 5, 2, 6, 1, 7)
FAR = (4, 3, -3, 2, -2, 1, -1, 0)
REQUEST_ORDER = (0, 1, -1, 2, -2, 3, -3, 4)
ROW_ORDER = (0, 1, -1, 2, -2, 3, -3, 4)
VMEM_LIMIT = 24 << 20
F32 = jnp.float32
BF16 = jnp.bfloat16


def dot(a, b):
    return jnp.dot(a, b, preferred_element_type=F32)


def dot_tn(a, b):
    return lax.dot_general(a, b, (((0,), (0,)), ((), ())), preferred_element_type=F32)


def dot_nt(a, b):
    return lax.dot_general(a, b, (((1,), (1,)), ((), ())), preferred_element_type=F32)


def iota(shape, dim):
    return lax.broadcasted_iota(jnp.int32, shape, dim)


def kernel_tile(columns, rows):
    squared = (columns[0] - rows[0]) ** 2
    squared = squared + (columns[1] - rows[1]) ** 2
    squared = squared + (columns[2] - rows[2]) ** 2
    return (kernel_scale * lax.rsqrt(squared + softening * softening)).astype(BF16)


def split3(values):
    high = values.astype(BF16).astype(F32)
    rest = values - high
    middle = rest.astype(BF16).astype(F32)
    return high, middle, rest - middle


def far_first(rows, cols):
    def wrapped(value, size):
        return (value + size // 2 - 1) % size - (size // 2 - 1)

    seen, groups = {(0, 0)}, []
    for a in range(rows):
        for b in range(cols):
            group = []
            for p, q in ((a, b), (-b, a), (-a, -b), (b, -a)):
                pair = (wrapped(p, rows), wrapped(q, cols))
                if pair not in seen:
                    seen.add(pair)
                    group.append(pair)
            if group:
                groups.append(group)
    groups.sort(key=lambda g: -(abs(g[0][0]) + abs(g[0][1])))
    flat = [pair for group in groups for pair in group]
    return sorted(flat, key=lambda p: -(2 * abs(p[0]) + abs(p[1])))


def level_kernel(
    nodes, reps, coords_hbm, omega_hbm, skel_hbm, row_ref, pin, spots,
    coords_ref, omega_ref, skel_ref, lists, reqs, asked, zreq, zasked, zout, zin, line, rout, rin, pout,
    nbc, nbw, own_t, own_wide, omega_t, table, acc, hot, scatter_hot, tile,
    gather_hot, load_sem, plane_sem, send_sem, recv_sem, asked_sem, nb_send, nb_recv,
):
    me, rep = lax.axis_index("node"), lax.axis_index("rep")
    leaf = coords_ref.shape[1]
    samp = omega_ref.shape[1]
    share = skel_ref.shape[1]
    rank_size = share * reps
    slots = nodes * CAP
    z, y, core = me // LINE, lax.rem(me // 2, LINE // 2), lax.rem(me, 2)
    spot = lax.rem(me, LINE)
    planes = nodes // LINE
    offsets = far_first(8, 8)

    def z_peer(d):
        return lax.rem(z + d, planes)

    def y_peer(d):
        return z * LINE + lax.rem(spot + d, LINE)

    barrier = pltpu.get_barrier_semaphore()

    loads = [
        pltpu.make_async_copy(src, dst, load_sem.at[k])
        for k, (src, dst) in enumerate(((skel_hbm, skel_ref), (coords_hbm, coords_ref), (omega_hbm, omega_ref)))
    ]
    for load in loads:
        load.start()

    def hello(node, column):
        pl.semaphore_signal(barrier, inc=1, device_id=(node, column), device_id_type=MESH)

    for d in Z_ORDER:
        hello(z_peer(d) * LINE + spot, rep)
    for d in Y_ORDER:
        hello(y_peer(d), rep)
    for d in range(1, reps):
        hello(me, lax.rem(rep + d, reps))
    for d in (1, nodes - 1):
        hello(lax.rem(me + d, nodes), rep)

    loads[0].wait()
    loads[1].wait()
    pl.semaphore_wait(barrier, reps - 1 + LINE - 1 + planes - 1 + 2)

    for d in range(1, reps):
        pltpu.make_async_remote_copy(
            src_ref=skel_ref, dst_ref=lists.at[rep], send_sem=send_sem.at[0], recv_sem=recv_sem.at[0],
            device_id=(me, lax.rem(rep + d, reps)), device_id_type=MESH,
        ).start()
    for d in Z_ORDER:
        pl.semaphore_signal(plane_sem, inc=1, device_id=(z_peer(d) * LINE + spot, rep), device_id_type=MESH)
    for d in Y_ORDER:
        pltpu.make_async_remote_copy(
            src_ref=coords_ref, dst_ref=line.at[spot], send_sem=send_sem.at[5], recv_sem=recv_sem.at[5],
            device_id=(y_peer(d), rep), device_id_type=MESH,
        ).start()

    nb_copies = []
    for side, step in ((0, 1), (1, nodes - 1)):
        for j, (src, dst) in enumerate(((coords_ref, nbc), (omega_ref, nbw))):
            nb_copies.append(
                pltpu.make_async_remote_copy(
                    src_ref=src, dst_ref=dst.at[side], send_sem=nb_send.at[side, j], recv_sem=nb_recv.at[side, j],
                    device_id=(lax.rem(me + step, nodes), rep), device_id_type=MESH,
                )
            )
    loads[2].wait()
    for copy in nb_copies:
        copy.start()

    lists[rep] = skel_ref[...]
    line[spot] = coords_ref[...]
    asked[me] = jnp.zeros((1, 128), F32)
    rin[me] = jnp.zeros((CAP, samp), BF16)
    pin[me] = jnp.zeros((CAP, samp), BF16)
    own = coords_ref[...]
    own_rows = [own[k : k + 1, :] for k in range(3)]
    own_t[...] = jnp.transpose(jnp.concatenate([own, jnp.zeros((128 - 3, leaf), F32)], axis=0))
    for k in range(3):
        own_wide[k] = jnp.broadcast_to(own_t[:, k : k + 1], (leaf, 128))

    def near(point_rows, sample_rows, first):
        @pl.loop(0, leaf // 128)
        def _(m):
            part = pl.ds(pl.multiple_of(m * 128, 128), 128)
            columns = [jnp.concatenate([own_wide[k, part, :]] * (leaf // 128), axis=1) for k in range(3)]
            term = dot(kernel_tile(columns, point_rows), sample_rows)
            acc[part, :] = term if first else acc[part, :] + term

    near(own_rows, omega_ref[...], True)

    def await_bytes(ref, count, sem):
        view = ref.at[pl.ds(0, count)]
        pltpu.make_async_copy(view, view, sem).wait()

    def send_to(src, dst, target, out_sem, in_sem):
        pltpu.make_async_remote_copy(
            src_ref=src.at[target], dst_ref=dst.at[me], send_sem=out_sem, recv_sem=in_sem,
            device_id=(target, rep), device_id_type=MESH,
        ).start()

    def send_pair(src, dst, chip, out_sem, in_sem, own_chip):
        if not own_chip:
            send_to(src, dst, chip + core, out_sem, in_sem)
        send_to(src, dst, chip + 1 - core, out_sem, in_sem)

    def exchange(src, dst, which):
        for dy, dz in offsets + [(0, 0)]:
            chip = lax.rem(z + (dz + 8), 8) * LINE + lax.rem(y + (dy + 8), 8) * 2
            send_pair(src, dst, chip, send_sem.at[which], recv_sem.at[which], dy == 0 and dz == 0)

    def z_exchange(src, dst, which):
        for d in Z_ORDER:
            pltpu.make_async_remote_copy(
                src_ref=src.at[z_peer(d)], dst_ref=dst.at[z], send_sem=send_sem.at[which], recv_sem=recv_sem.at[which],
                device_id=(z_peer(d) * LINE + spot, rep), device_id_type=MESH,
            ).start()

    await_bytes(lists, reps - 1, recv_sem.at[0])

    listed = jnp.concatenate([lists[r] for r in range(reps)], axis=1)
    owner_row = listed >> 9
    listed_col = jnp.transpose(jnp.broadcast_to(listed.astype(F32), (128, rank_size))).astype(jnp.int32)
    owner_col = listed_col >> 9
    value_col = (listed_col & (leaf - 1)) + 1
    wide_owner = jnp.concatenate([owner_col] * (rank_size // 128), axis=1)
    same = wide_owner == owner_row
    before = jnp.where(same & (iota(same.shape, 1) < iota(same.shape, 0)), 1.0, 0.0).astype(BF16)
    rank_col = dot(before, jnp.ones((rank_size, 128), BF16)).astype(jnp.int32)
    low_col = (value_col & 255).astype(F32)
    high_col = (value_col >> 8).astype(F32)

    def requests(lane_col, owner_hot):
        placed = lane_col == iota((rank_size, 128), 1)
        low = jnp.where(placed, low_col, 0.0).astype(BF16)
        high = jnp.where(placed, high_col, 0.0).astype(BF16)
        return dot(owner_hot, low) + 256.0 * dot(owner_hot, high)

    z_hot = jnp.where((owner_row >> 4) == iota((16, rank_size), 0), 1.0, 0.0).astype(BF16)
    z_request = requests((owner_col & (LINE - 1)) * CAP + rank_col, z_hot)
    for i in range(planes):
        zreq[i] = z_request[i : i + 1, :]
    z_exchange(zreq, zasked, 2)
    zasked[z] = zreq[z]

    owner_hot = jnp.where(owner_row == iota((nodes, rank_size), 0), 1.0, 0.0).astype(BF16)
    reqs[...] = requests(rank_col, owner_hot).reshape(nodes, 1, 128)
    pl.semaphore_wait(plane_sem, planes - 1)
    for dz in REQUEST_ORDER:
        base = z_peer(planes + dz) * LINE
        for dy in FAR:
            chip = base + lax.rem(y + (dy + 8), 8) * 2
            send_pair(reqs, asked, chip, send_sem.at[1], asked_sem.at[z], dy == 0 and dz == 0)

    await_bytes(line, LINE - 1, recv_sem.at[5])
    for k in range(3):
        for part, values in enumerate(split3(jnp.concatenate([line[n, k : k + 1, :] for n in range(LINE)], axis=0))):
            table[pl.ds((3 * k + part) * LINE, LINE), :] = values.astype(BF16)

    flat_col = owner_col * CAP + rank_col
    flat_wide = jnp.concatenate([flat_col] * (slots // 128), axis=1)
    gather_hot[...] = jnp.where(flat_wide == iota((rank_size, slots), 1), 1.0, 0.0).astype(BF16)
    earlier = jnp.where(same & (iota(same.shape, 0) < iota(same.shape, 1)), 1.0, 0.0)
    rank_row = jnp.sum(earlier, axis=0, keepdims=True).astype(jnp.int32)
    flat_row = owner_row * CAP + rank_row
    scatter_hot[...] = jnp.where(flat_row == iota((slots, rank_size), 0), 1.0, 0.0).astype(BF16)

    omega_t[...] = jnp.transpose(omega_ref[...])

    await_bytes(zasked, planes - 1, recv_sem.at[2])
    width = 256
    for c in range(slots // width):
        wanted = jnp.concatenate([zasked[2 * c], zasked[2 * c + 1]], axis=1)
        point_hot = jnp.where(wanted == (iota((leaf, width), 0) + 1).astype(F32), 1.0, 0.0).astype(BF16)
        found = dot(table[...], point_hot)
        own_node = lax.rem(iota((3 * LINE, width), 0), LINE) == lax.rem(iota((3 * LINE, width), 1) // CAP, LINE)
        answer = jnp.concatenate(
            [
                jnp.sum(jnp.where(own_node, found[3 * LINE * k : 3 * LINE * (k + 1)], 0.0), axis=0, keepdims=True)
                for k in range(3)
            ],
            axis=0,
        )
        zout[2 * c] = answer[:, :128]
        zout[2 * c + 1] = answer[:, 128:]
    z_exchange(zout, zin, 6)
    zin[z] = zout[z]

    point = (iota((LINE * CAP, leaf), 1) + 1).astype(F32)
    for dz in ROW_ORDER:
        zs = z_peer(planes + dz)
        nodes_of = pl.ds(pl.multiple_of(zs * LINE, LINE), LINE)
        slots_of = pl.ds(pl.multiple_of(zs * LINE * CAP, LINE * CAP), LINE * CAP)
        await_bytes(asked, LINE if dz else LINE - 1, asked_sem.at[zs])
        spread = jnp.broadcast_to(asked[nodes_of], (LINE, CAP, 128))
        spread = jnp.where(iota(spread.shape, 2) == iota(spread.shape, 1), spread, 0.0)
        flat = jnp.sum(spread.reshape(LINE * CAP, 128), axis=1, keepdims=True)
        point_hot = jnp.where(flat == point, 1.0, 0.0).astype(BF16)
        hot[slots_of, :] = point_hot
        rout[nodes_of] = dot(point_hot, omega_ref[...]).reshape(LINE, CAP, samp).astype(BF16)
        for dy in FAR:
            chip = zs * LINE + lax.rem(y + (dy + 8), 8) * 2
            send_pair(rout, rin, chip, send_sem.at[3], recv_sem.at[3], dy == 0 and dz == 0)

    for copy in nb_copies:
        copy.wait_recv()

    @pl.when(me > 0)
    def _():
        side = nbc[0]
        near([side[k : k + 1, :] for k in range(3)], nbw[0], False)

    def send_products():
        await_bytes(zin, planes - 1, recv_sem.at[6])
        points = jnp.concatenate([zin[i] for i in range(planes)], axis=1)
        points = jnp.concatenate([points, jnp.zeros((5, slots), F32)], axis=0)
        parts = jnp.concatenate(split3(points) + (jnp.zeros((8, slots), F32),), axis=0).astype(BF16)
        picked = dot(parts, scatter_hot[...])
        skel = picked[0:8] + picked[8:16] + picked[16:24]
        skel_rows = [skel[k : k + 1, :] for k in range(3)]
        for m in range(leaf // 128):
            part = pl.ds(m * 128, 128)
            columns = [jnp.concatenate([own_wide[k, part, :]] * (rank_size // 128), axis=1) for k in range(3)]
            tile[part, :] = kernel_tile(columns, skel_rows)
        transposed = dot(omega_t[...], tile[...]).astype(BF16)
        pout[...] = dot_nt(scatter_hot[...], transposed).reshape(nodes, CAP, samp).astype(BF16)
        exchange(pout, pin, 4)

    send_products()

    @pl.when(me < nodes - 1)
    def _():
        side = nbc[1]
        near([side[k : k + 1, :] for k in range(3)], nbw[1], False)

    spots[...] = jnp.transpose(hot[...])

    await_bytes(rin, nodes - 1, recv_sem.at[3])
    got = rin[...].astype(F32).reshape(slots, samp).astype(BF16)
    skel_samples = dot(gather_hot[...], got).astype(BF16)
    row_ref[...] = (acc[...] + dot(tile[...], skel_samples)).astype(BF16)

    await_bytes(lists, reps - 1, send_sem.at[0])
    await_bytes(line, LINE - 1, send_sem.at[5])
    for which, ref in ((1, reqs), (3, rout), (4, pout)):
        await_bytes(ref, nodes - 1, send_sem.at[which])
    for which, ref in ((2, zreq), (6, zout)):
        await_bytes(ref, planes - 1, send_sem.at[which])
    for copy in nb_copies:
        copy.wait_send()
    await_bytes(pin, nodes - 1, recv_sem.at[4])


def finish_kernel(row_ref, pin, spots, row_hbm, col_hbm, incoming, col_ref, sems):
    leaf = row_ref.shape[0]
    copies = [pltpu.make_async_copy(row_ref, row_hbm, sems.at[0])]
    copies[0].start()
    incoming[...] = pin[...].astype(F32).reshape(incoming.shape).astype(BF16)
    step = leaf // 2
    for k in range(2):
        part = pl.ds(k * step, step)
        col_ref[part, :] = dot(spots[part, :], incoming[...])
        copies.append(pltpu.make_async_copy(col_ref.at[part], col_hbm.at[part], sems.at[1 + k]))
        copies[-1].start()
    for copy in copies:
        copy.wait()


def solution(mesh):
    nodes, reps = mesh.shape["node"], mesh.shape["rep"]

    def on_device(coords, omega, skeleton):
        leaf, samp = omega.shape
        share = skeleton.shape[1]
        vmem = pl.BlockSpec(memory_space=pltpu.VMEM)
        anywhere = pl.BlockSpec(memory_space=pl.ANY)
        row, incoming, spots = pl.pallas_call(
            functools.partial(level_kernel, nodes, reps),
            out_shape=(
                jax.ShapeDtypeStruct((leaf, samp), BF16),
                jax.ShapeDtypeStruct((nodes, CAP, samp), BF16),
                jax.ShapeDtypeStruct((leaf, nodes * CAP), BF16),
            ),
            in_specs=[pl.BlockSpec(memory_space=pltpu.HBM)] * 3,
            out_specs=(vmem,) * 3,
            scratch_shapes=[
                pltpu.VMEM(coords.shape, F32),
                pltpu.VMEM((leaf, samp), BF16),
                pltpu.VMEM((1, share), jnp.int32),
                pltpu.VMEM((reps, 1, share), jnp.int32),
                pltpu.VMEM((nodes, 1, 128), F32),
                pltpu.VMEM((nodes, 1, 128), F32),
                pltpu.VMEM((nodes // LINE, 1, 128), F32),
                pltpu.VMEM((nodes // LINE, 1, 128), F32),
                pltpu.VMEM((nodes // LINE, 3, 128), F32),
                pltpu.VMEM((nodes // LINE, 3, 128), F32),
                pltpu.VMEM((LINE, 3, leaf), F32),
                pltpu.VMEM((nodes, CAP, samp), BF16),
                pltpu.VMEM((nodes, CAP, samp), BF16),
                pltpu.VMEM((nodes, CAP, samp), BF16),
                pltpu.VMEM((2, 3, leaf), F32),
                pltpu.VMEM((2, leaf, samp), BF16),
                pltpu.VMEM((leaf, 128), F32),
                pltpu.VMEM((3, leaf, 128), F32),
                pltpu.VMEM((samp, leaf), BF16),
                pltpu.VMEM((9 * LINE, leaf), BF16),
                pltpu.VMEM((leaf, samp), F32),
                pltpu.VMEM((nodes * CAP, leaf), BF16),
                pltpu.VMEM((nodes * CAP, share * reps), BF16),
                pltpu.VMEM((leaf, share * reps), BF16),
                pltpu.VMEM((share * reps, nodes * CAP), BF16),
                pltpu.SemaphoreType.DMA((3,)),
                pltpu.SemaphoreType.REGULAR,
                pltpu.SemaphoreType.DMA((7,)),
                pltpu.SemaphoreType.DMA((7,)),
                pltpu.SemaphoreType.DMA((nodes // LINE,)),
                pltpu.SemaphoreType.DMA((2, 2)),
                pltpu.SemaphoreType.DMA((2, 2)),
            ],
            compiler_params=pltpu.CompilerParams(
                collective_id=0, has_side_effects=True, vmem_limit_bytes=VMEM_LIMIT
            ),
        )(*(pltpu.with_memory_space_constraint(a, pltpu.HBM) for a in (coords, omega, skeleton)))
        return pl.pallas_call(
            finish_kernel,
            out_shape=(
                jax.ShapeDtypeStruct((leaf, samp), BF16),
                jax.ShapeDtypeStruct((leaf, samp), F32),
            ),
            in_specs=[vmem] * 3,
            out_specs=(anywhere,) * 2,
            scratch_shapes=[
                pltpu.VMEM((nodes * CAP, samp), BF16),
                pltpu.VMEM((leaf, samp), F32),
                pltpu.SemaphoreType.DMA((3,)),
            ],
            compiler_params=pltpu.CompilerParams(vmem_limit_bytes=VMEM_LIMIT),
        )(row, incoming, spots)

    return jax.shard_map(
        on_device,
        mesh=mesh,
        in_specs=(P(None, "node"), P("node", "rep"), P("node", "rep")),
        out_specs=(P("node", "rep"), P("node", "rep")),
        check_vma=False,
    )
```
